256 devices in a mesh: section: 16 (over z, x_lo), fsdp: 16 (over x_hi, y, core).
Axes of the slice: x: 4 (x_hi: 2, x_lo: 2; x = x_hi * 2 + x_lo), y: 4, z: 8, core: 2. Of those that a mesh axis runs over, the one named last changes fastest.
Arguments:
- layer_inputs: bfloat16 [16, 2, 6144, 2048], P('section', None, 'fsdp'), may hold values from -6 to 6
- out_grads: bfloat16 [16, 2, 6144, 2048], P('section', None, 'fsdp'), may hold values from -6 to 6
- attn_stash: bfloat16 [16, 2, 6144, 1024], P('section', None, 'fsdp'), may hold values from -6 to 6
- proj_grads: bfloat16 [16, 2, 6144, 1536], P('section', None, 'fsdp'), may hold values from -6 to 6
- w_qkv: bfloat16 [16, 2048, 1536], P('section', 'fsdp'), may hold values from -0.125 to 0.125
- w_out: bfloat16 [16, 1024, 2048], P('section', 'fsdp'), may hold values from -0.1875 to 0.1875
- norm_gain: float32 [16, 2048], P('section'), may hold values from 0.25 to 1.75
- b_sched: int32 [16], P('section'), may hold values from 0 to 1
- w_sched: int32 [16], P('section'), may hold values from 0 to 1
Outputs:
- prev_grads: bfloat16 [16, 6144, 2048], P('section', 'fsdp')
- grad_qkv: float32 [16, 2048, 1536], P('section', 'fsdp')
- grad_out: float32 [16, 1024, 2048], P('section', 'fsdp')
The draws below stay inside these ranges and needn't reach their ends.
All inputs are finite; a program needn't handle non-finite values.
Results may differ from the reference program's by a relative error of at most 0.012.
Values may be sent and summed in bfloat16 or wider, within the bound.
A program may use at most 128 MiB of HBM per device.

```python
import jax
import jax.numpy as jnp
from jax import lax

D = 2048
HEAD_DIM = 64
HEADS = 16
KV_HEADS = 4
SEQ = 384
MICRO = 2
SECTIONS = 16
Q_WIDTH = 1024
QKV_WIDTH = 1536
TOKENS = 6144
N_FSDP = 16


def set_ends(values, own_key, smallest, top_value):
    longest = values.shape.index(max(values.shape))
    spots = []
    for shift in (0, 1):
        where = [jax.random.randint(jax.random.fold_in(own_key, axis), (), 0, length) for axis, length in enumerate(values.shape)]
        where[longest] = (where[longest] + shift) % values.shape[longest]
        spots.append(tuple(where))
    return values.at[spots[0]].set(smallest).at[spots[1]].set(top_value)


def raised(values, stream_key, source, target, parts, factor):
    owner, partner = [(jnp.arange(values.shape[position]) // (values.shape[position] // parts)).reshape([-1 if axis == position else 1 for axis in range(values.ndim)]) for position in (source, target)]
    chosen = jax.random.permutation(stream_key, parts)[partner]
    strong = (owner == chosen) | (owner == (partner + parts // 2) % parts)
    return jnp.where(strong, factor * values, values)


def level_of(own_key, shape, cuts, smallest, high):
    def one(axis_at, blocks):
        steps = jax.random.uniform(jax.random.fold_in(jax.random.fold_in(own_key, 6), axis_at), (blocks,), jnp.float32, smallest / len(cuts), high / len(cuts))
        return jnp.repeat(jnp.exp(steps), shape[axis_at] // blocks).reshape((-1,) + (1,) * (len(shape) - axis_at - 1))

    loudness = one(*cuts[0])
    for cut in cuts[1:]:
        loudness = loudness * one(*cut)
    return loudness


def scatter_about(stream_key, dims, scale, bound, pieces=(), kind=jnp.bfloat16):
    loudness = level_of(stream_key, dims, pieces, -0.22, 0.18) if pieces else 1.0
    entries = jax.random.normal(stream_key, dims, jnp.float32) * scale * loudness
    return jnp.minimum(jnp.maximum(entries, -bound), bound).astype(kind)


def heavy_noise(key, dims, spread, most, pieces, heavy, kind=jnp.bfloat16):
    entries = spread * jax.random.normal(key, dims, jnp.float32)
    if pieces:
        entries = entries * level_of(key, dims, pieces, -0.22, 0.18)
    return jnp.clip(raised(entries, jax.random.fold_in(key, 3), *heavy), -most, most).astype(kind)


def setup_inputs(seed: int = 0) -> dict:
    streams_of = jax.random.split(jax.random.key(seed), 10)
    layer_inputs = scatter_about(streams_of[0], (SECTIONS, MICRO, TOKENS, D), 1.0, 6.0, ((0, 16), (2, 16)))
    out_grads = scatter_about(streams_of[1], (SECTIONS, MICRO, TOKENS, D), 1.0, 6.0, ((0, 16), (2, 16)))
    attn_stash = heavy_noise(streams_of[2], (SECTIONS, MICRO, TOKENS, Q_WIDTH), 1.0, 6.0, ((0, 16), (2, 16)), (2, 3, 16, 2.0))
    proj_grads = scatter_about(streams_of[3], (SECTIONS, MICRO, TOKENS, QKV_WIDTH), 1.0, 6.0, ((0, 16), (2, 16)))
    w_qkv = scatter_about(streams_of[4], (SECTIONS, D, QKV_WIDTH), D ** -0.5, 0.125, ((0, 16), (1, 16)))
    w_out = scatter_about(streams_of[5], (SECTIONS, Q_WIDTH, D), Q_WIDTH ** -0.5, 0.1875, ((0, 16), (1, 16)))
    norm_gain = jnp.clip(1.0 + 0.15 * jax.random.normal(streams_of[6], (SECTIONS, D), jnp.float32), 0.25, 1.75)
    b_sched = set_ends(jax.random.randint(streams_of[7], (SECTIONS,), 0, MICRO), jax.random.fold_in(streams_of[7], 1), 0, MICRO - 1).astype(jnp.int32)
    w_sched = set_ends(jax.random.randint(streams_of[8], (SECTIONS,), 0, MICRO), jax.random.fold_in(streams_of[8], 1), 0, MICRO - 1).astype(jnp.int32)
    return dict(layer_inputs=layer_inputs, out_grads=out_grads, attn_stash=attn_stash, proj_grads=proj_grads, w_qkv=w_qkv, w_out=w_out, norm_gain=norm_gain, b_sched=b_sched, w_sched=w_sched)


rms_eps = 1e-05
rope_base = 500000.0

def rope_tables(length, head_size):
    halfway = head_size // 2
    indices = jnp.arange(halfway, dtype=jnp.float32)
    frequency = rope_base ** (-2.0 * indices / head_size)
    angles = jnp.arange(length, dtype=jnp.float32)[:, None] * frequency[None, :]
    angles = jnp.concatenate([angles, angles], axis=1)
    return (jnp.cos(angles), jnp.sin(angles))

def rotate_half(values):
    halfway = values.shape[-1] // 2
    return jnp.concatenate([-values[..., halfway:], values[..., :halfway]], axis=-1)

def apply_rope(values, cosine_table, sine_table):
    return values * cosine_table[:, None, :] + rotate_half(values) * sine_table[:, None, :]

def unapply_rope(values, cosine_table, sine_table):
    return values * cosine_table[:, None, :] - rotate_half(values * sine_table[:, None, :])

def contract(pattern, first_operand, second_operand):
    return jnp.einsum(pattern, first_operand.astype(jnp.float32), second_operand.astype(jnp.float32))

def normalize(inputs, gain_values):
    widened = inputs.astype(jnp.float32)
    inv_rms = lax.rsqrt(lax.optimization_barrier(jnp.mean(widened * widened, axis=-1, keepdims=True)) + rms_eps)
    normed = (widened * inv_rms * gain_values).astype(jnp.bfloat16)
    return (widened, inv_rms, normed)

def attention_back(qkv_rows, attn_grad, cosine_table, sine_table):
    tokens_here = qkv_rows.shape[0]
    q_width = HEADS * HEAD_DIM
    kv_width = KV_HEADS * HEAD_DIM
    group_size = HEADS // KV_HEADS
    score_scale = HEAD_DIM ** (-0.5)
    queries = apply_rope(qkv_rows[:, :q_width].reshape(tokens_here, HEADS, HEAD_DIM), cosine_table, sine_table).astype(jnp.bfloat16)
    key_heads = apply_rope(qkv_rows[:, q_width:q_width + kv_width].reshape(tokens_here, KV_HEADS, HEAD_DIM), cosine_table, sine_table).astype(jnp.bfloat16)
    values = qkv_rows[:, q_width + kv_width:].reshape(tokens_here, KV_HEADS, HEAD_DIM).astype(jnp.bfloat16)
    queries = queries.reshape(tokens_here, KV_HEADS, group_size, HEAD_DIM)
    grad_heads = attn_grad.reshape(tokens_here, KV_HEADS, group_size, HEAD_DIM)
    scores = contract('tkgd,ukd->kgtu', queries, key_heads) * score_scale
    row_ids = lax.broadcasted_iota(jnp.int32, (tokens_here, tokens_here), 0)
    col_ids = lax.broadcasted_iota(jnp.int32, (tokens_here, tokens_here), 1)
    causal = col_ids <= row_ids
    exp_scores = jnp.where(causal, jnp.exp(scores), 0.0)
    attention = exp_scores / lax.optimization_barrier(jnp.sum(exp_scores, axis=-1, keepdims=True))
    attention_low = attention.astype(jnp.bfloat16)
    grad_values = contract('kgtu,tkgd->ukd', attention_low, grad_heads)
    grad_attention = contract('tkgd,ukd->kgtu', grad_heads, values)
    row_delta = lax.optimization_barrier(jnp.sum(attention * grad_attention, axis=-1, keepdims=True))
    grad_scores = (attention * (grad_attention - row_delta) * score_scale).astype(jnp.bfloat16)
    grad_queries = contract('kgtu,ukd->tkgd', grad_scores, key_heads)
    grad_keys = contract('kgtu,tkgd->ukd', grad_scores, queries)
    grad_queries = unapply_rope(grad_queries.reshape(tokens_here, HEADS, HEAD_DIM), cosine_table, sine_table)
    grad_keys = unapply_rope(grad_keys, cosine_table, sine_table)
    joined = jnp.concatenate([grad_queries.reshape(tokens_here, q_width), grad_keys.reshape(tokens_here, kv_width), grad_values.reshape(tokens_here, kv_width)], axis=1)
    return joined.astype(jnp.bfloat16)

def finish_grad(widened, inv_rms, gain_values, upstream, grad_normed):
    scaled = grad_normed * gain_values
    inner_mean = lax.optimization_barrier(jnp.mean(scaled * widened, axis=-1, keepdims=True))
    result = upstream.astype(jnp.float32) + inv_rms * scaled - widened * inv_rms ** 3 * inner_mean
    return result.astype(jnp.bfloat16)

def reference(layer_inputs, out_grads, attn_stash, proj_grads, w_qkv, w_out, norm_gain, b_sched, w_sched):
    cosine_table, sine_table = rope_tables(SEQ, HEAD_DIM)
    contract_rows = (((0,), (0,)), ((), ()))
    contract_cols = (((1,), (1,)), ((), ()))

    def one_section(operands):
        inputs, upstream, attended, projected, weight_qkv, weight_out, gain_values, b_slot, w_slot = operands
        inputs_b = lax.dynamic_index_in_dim(inputs, b_slot, 0, keepdims=False).reshape(N_FSDP, SEQ, D)
        upstream_b = lax.dynamic_index_in_dim(upstream, b_slot, 0, keepdims=False).reshape(N_FSDP, SEQ, D)

        def one_sequence(seq_pair):
            seq_inputs, seq_upstream = seq_pair
            widened, inv_rms, normed = normalize(seq_inputs, gain_values)
            qkv_rows = jnp.dot(normed, weight_qkv, preferred_element_type=jnp.float32)
            attn_grad = lax.dot_general(seq_upstream, weight_out, contract_cols, preferred_element_type=jnp.float32).astype(jnp.bfloat16)
            grad_proj = attention_back(qkv_rows, attn_grad, cosine_table, sine_table)
            grad_normed = lax.dot_general(grad_proj, weight_qkv, contract_cols, preferred_element_type=jnp.float32)
            return finish_grad(widened, inv_rms, gain_values, seq_upstream, grad_normed)
        sent_grads = lax.map(one_sequence, (inputs_b, upstream_b)).reshape(TOKENS, D)
        inputs_w = lax.dynamic_index_in_dim(inputs, w_slot, 0, keepdims=False).reshape(N_FSDP, SEQ, D)
        upstream_w = lax.dynamic_index_in_dim(upstream, w_slot, 0, keepdims=False).reshape(N_FSDP, SEQ, D)
        attended_w = lax.dynamic_index_in_dim(attended, w_slot, 0, keepdims=False).reshape(N_FSDP, SEQ, Q_WIDTH)
        projected_w = lax.dynamic_index_in_dim(projected, w_slot, 0, keepdims=False).reshape(N_FSDP, SEQ, QKV_WIDTH)

        def add_member(totals, member):
            m_inputs, m_upstream, m_attended, m_projected = member
            unused_wide, unused_inv, normed = normalize(m_inputs, gain_values)
            part_qkv = lax.dot_general(normed, m_projected, contract_rows, preferred_element_type=jnp.float32)
            part_out = lax.dot_general(m_attended, m_upstream, contract_rows, preferred_element_type=jnp.float32)
            part_qkv = lax.optimization_barrier(part_qkv.astype(jnp.bfloat16)).astype(jnp.float32)
            part_out = lax.optimization_barrier(part_out.astype(jnp.bfloat16)).astype(jnp.float32)
            return ((totals[0] + part_qkv, totals[1] + part_out), None)
        zero_totals = (jnp.zeros((D, QKV_WIDTH), jnp.float32), jnp.zeros((Q_WIDTH, D), jnp.float32))
        grad_pair, unused_out = lax.scan(add_member, zero_totals, (inputs_w, upstream_w, attended_w, projected_w))
        return (sent_grads, grad_pair[0], grad_pair[1])
    sent_all, grad_qkv, grad_out = lax.map(one_section, (layer_inputs, out_grads, attn_stash, proj_grads, w_qkv, w_out, norm_gain, b_sched, w_sched))
    return (jnp.roll(sent_all, -1, axis=0), grad_qkv, grad_out)
```

```python
import functools

import jax
import jax.numpy as jnp
import numpy as np
from jax import lax
from jax.experimental import pallas as pl
from jax.experimental.pallas import tpu as pltpu
from jax.sharding import PartitionSpec as P

D = 2048
HEAD_DIM = 64
HEADS = 16
KV_HEADS = 4
SEQ = 384
QW = 1024
QKVW = 1536
CHIPS = 8
EPS = 1e-05
SCALE = HEAD_DIM ** (-0.5)
BF = jnp.bfloat16
F32 = jnp.float32
MESH = pl.DeviceIdType.MESH

Q_X, Q_YP, Q_YM, Q_PP, Q_PM, Q_RO, Q_RP = range(7)
O_YP, O_YM, O_X0, O_XP, O_XM, O_X2, O_RA, O_RB = range(7, 15)
SIB_Q = 15
SIB_O = 23
RS_SIB_Q, RS_SIB_O = 31, 32
R1_Q, R1_O = 33, 35
R2_Q, R2_O = 37, 41
RX_Q, RX_O = 45, 46
PERM = 47
N_SEM = 50


def rope_tables():
    half = HEAD_DIM // 2
    freq = 500000.0 ** (-2.0 * np.arange(half) / HEAD_DIM)
    ang = np.arange(SEQ)[:, None] * freq[None, :]
    cos = np.tile(np.cos(ang), (1, 4)).astype(np.float32)
    sin = np.tile(np.sin(ang), (1, 4)).astype(np.float32)
    sign = np.where(np.arange(128) % 64 < 32, -1.0, 1.0).astype(np.float32)
    return cos, sin * sign[None, :]


def dot(a, b, ca, cb):
    return lax.dot_general(a, b, (((ca,), (cb,)), ((), ())), preferred_element_type=F32)


def kernel(
    x_hbm, g_hbm, a_hbm, p_hbm, wq_hbm, wo_hbm, gain_ref, b_ref, w_ref, cos_ref, sin_ref,
    prev_hbm, gq_ref, go_ref,
    X, G, A, PG, WQ, WO, DQ, DO, SQ, SO, R1Q, R1O, R2Q, R2O, RXQ, RXO,
    N, INV, Q, KD, VD, AGR, GP, DKD, DVD, U, DOT, OUT,
    lsem, ssem, rsem,
):
    s = lax.axis_index("section")
    f = lax.axis_index("fsdp")
    xh, y, c = f // 8, (f // 2) % 4, f % 2
    up, down, far = (y + 1) % 4, (y + 3) % 4, (y + 2) % 4
    oc, ox = 1 - c, 1 - xh
    n_sec = lax.axis_size("section")

    def dev(xx, yy, cc):
        return (s, xx * 8 + yy * 2 + cc)

    d_up, d_down, d_x, d_sib = dev(xh, up, c), dev(xh, down, c), dev(ox, y, c), dev(xh, y, oc)
    d_prev, d_next = (lax.rem(s + n_sec - 1, n_sec), f), (lax.rem(s + 1, n_sec), f)

    def qs(ref, xx, yy, cc):
        return ref.at[xx * 4 + yy, pl.ds(pl.multiple_of(cc * 128, 128), 128), :]

    def os(ref, xx, yy, cc, lo=0, n=64):
        return ref.at[xx * 4 + yy, pl.ds(pl.multiple_of(cc * 64 + lo, 32), n), :]

    started = []

    def rcopy(src, dst, slot, device):
        return pltpu.make_async_remote_copy(
            src_ref=src, dst_ref=dst, send_sem=ssem.at[slot], recv_sem=rsem.at[slot],
            device_id=device, device_id_type=MESH,
        )

    def send(src, dst, slot, device):
        cp = rcopy(src, dst, slot, device)
        cp.start()
        started.append(cp)

    def recv(dst, slot):
        rcopy(dst, dst, slot, d_sib).wait_recv()

    def gather(ref, shard, slot, device, src=None):
        send(shard if src is None else src, shard, slot, device)

    barrier = pltpu.get_barrier_semaphore()
    for d in (d_up, d_down, d_x, d_sib, d_prev, d_next):
        pl.semaphore_signal(barrier, inc=1, device_id=d, device_id_type=MESH)
    loads = [
        pltpu.make_async_copy(g_hbm, G, lsem.at[0]),
        pltpu.make_async_copy(a_hbm, A, lsem.at[1]),
        pltpu.make_async_copy(x_hbm, X, lsem.at[2]),
        pltpu.make_async_copy(p_hbm, PG, lsem.at[3]),
        pltpu.make_async_copy(wq_hbm, qs(WQ, xh, y, c), lsem.at[4]),
        pltpu.make_async_copy(wo_hbm, os(WO, xh, y, c), lsem.at[5]),
    ]
    for cp in (loads[4], loads[5], loads[0], loads[1], loads[2], loads[3]):
        cp.start()
    pl.semaphore_wait(barrier, 6)

    mine_q, mine_o = qs(WQ, xh, y, c), os(WO, xh, y, c)
    gather(WQ, mine_q, Q_X, d_x, wq_hbm)
    gather(WQ, mine_q, Q_YP, d_up, wq_hbm)
    gather(WQ, mine_q, Q_YM, d_down, wq_hbm)
    gather(WO, mine_o, O_YP, d_up, wo_hbm)
    gather(WO, mine_o, O_YM, d_down, wo_hbm)
    gather(WO, mine_o, O_X0, d_x, wo_hbm)
    gather(WQ, mine_q, SIB_Q + 0, d_sib, wq_hbm)
    gather(WO, mine_o, SIB_O + 0, d_sib, wo_hbm)

    b_slot, w_slot = b_ref[0], w_ref[0]

    loads[0].wait()
    loads[1].wait()

    def out_part(j, carry):
        lhs = A[w_slot, :, pl.ds(pl.multiple_of(j * 256, 256), 256)]

        def cols(n, carry):
            sl = pl.ds(pl.multiple_of(n * 512, 512), 512)
            part = dot(lhs, G[w_slot, :, sl], 0, 0).astype(BF)
            DO[pl.ds(2 * j, 2), :, sl] = part.reshape(2, 128, 512)
            return carry

        return lax.fori_loop(0, 4, cols, carry)

    lax.fori_loop(0, 4, out_part, 0)
    loads[2].wait()
    loads[3].wait()

    def norm(slot):
        def rows(r, carry):
            sl = pl.ds(pl.multiple_of(r * 16, 16), 16)
            wide = X[slot, sl, :].astype(F32)
            inv = lax.rsqrt(jnp.mean(wide * wide, axis=-1, keepdims=True) + EPS)
            INV[sl, :] = jnp.broadcast_to(inv, (16, 128))
            N[sl, :] = (wide * inv * gain_ref[...]).astype(BF)
            return carry

        lax.fori_loop(0, SEQ // 16, rows, 0)

    norm(w_slot)

    def qkv_part(j, carry):
        lhs = N[:, pl.ds(pl.multiple_of(j * 256, 256), 256)]

        def cols(n, carry):
            sl = pl.ds(pl.multiple_of(n * 512, 512), 512)
            DQ[j, :, sl] = dot(lhs, PG[w_slot, :, sl], 0, 0).astype(BF)
            return carry

        return lax.fori_loop(0, 3, cols, carry)

    lax.fori_loop(0, CHIPS, qkv_part, 0)
    norm(b_slot)
    send(DQ.at[:, pl.ds(pl.multiple_of(oc * 128, 128), 128), :], SQ, RS_SIB_Q, d_sib)
    send(DO.at[:, pl.ds(pl.multiple_of(oc * 64, 64), 64), :], SO, RS_SIB_O, d_sib)

    sgn = 1 - 2 * xh
    ya, yb = (y + 4 - sgn) % 4, (y + 4 + sgn) % 4
    part_q = qs(WQ, ox, y, c)
    recv(part_q, Q_X)
    gather(WQ, part_q, Q_PP, d_up)
    gather(WQ, part_q, Q_PM, d_down)
    gather(WQ, part_q, SIB_Q + 1, d_sib)
    from_down, from_up = qs(WQ, xh, down, c), qs(WQ, xh, up, c)
    recv(from_down, Q_YP)
    recv(from_up, Q_YM)
    gather(WQ, from_down, SIB_Q + 2, d_sib)
    gather(WQ, from_up, SIB_Q + 3, d_sib)
    o_down, o_up = os(WO, xh, down, c), os(WO, xh, up, c)
    recv(o_down, O_YP)
    recv(o_up, O_YM)
    gather(WO, os(WO, xh, down, c, 0, 32), O_RA, d_up)
    gather(WO, os(WO, xh, up, c, 32, 32), O_RB, d_down)
    gather(WO, o_down, O_XP, d_x)
    gather(WO, o_up, O_XM, d_x)
    gather(WO, o_down, SIB_O + 1, d_sib)
    gather(WO, o_up, SIB_O + 2, d_sib)
    gather(WQ, qs(WQ, xh, ya, c), Q_RO, dev(xh, yb, c))

    recv(SQ, RS_SIB_Q)
    recv(SO, RS_SIB_O)

    def pair_sum(j, carry):
        sq = pl.ds(pl.multiple_of(c * 128, 128), 128)
        so = pl.ds(pl.multiple_of(c * 64, 64), 64)
        DQ[j, sq, :] = (DQ[j, sq, :].astype(F32) + SQ[j].astype(F32)).astype(BF)
        DO[j, so, :] = (DO[j, so, :].astype(F32) + SO[j].astype(F32)).astype(BF)
        return carry

    lax.fori_loop(0, CHIPS, pair_sum, 0)

    part_down, part_up = qs(WQ, ox, down, c), qs(WQ, ox, up, c)
    recv(part_down, Q_PP)
    recv(part_up, Q_PM)
    gather(WQ, qs(WQ, ox, yb, c), Q_RP, dev(xh, ya, c))
    gather(WQ, part_down, SIB_Q + 4, d_sib)
    gather(WQ, part_up, SIB_Q + 5, d_sib)

    send(qs(DQ, 0, far, c), R1Q.at[0], R1_Q + 0, d_up)
    send(qs(DQ, 1, far, c), R1Q.at[1], R1_Q + 1, d_down)
    send(os(DO, 0, far, c), R1O.at[0], R1_O + 0, d_up)
    send(os(DO, 1, far, c), R1O.at[1], R1_O + 1, d_down)
    send(qs(DQ, 1, up, c), R2Q.at[0, 1], R2_Q + 1, d_up)
    send(qs(DQ, 0, down, c), R2Q.at[1, 0], R2_Q + 2, d_down)

    o_far = os(WO, xh, far, c)
    recv(os(WO, xh, far, c, 0, 32), O_RA)
    recv(os(WO, xh, far, c, 32, 32), O_RB)
    gather(WO, o_far, O_X2, d_x)
    gather(WO, o_far, SIB_O + 3, d_sib)
    for i, (yy, slot) in enumerate(((y, O_X0), (down, O_XP), (up, O_XM), (far, O_X2))):
        piece = os(WO, ox, yy, c)
        recv(piece, slot)
        gather(WO, piece, SIB_O + 4 + i, d_sib)
    far_own, far_part = qs(WQ, xh, far, c), qs(WQ, ox, far, c)
    recv(far_own, Q_RO)
    gather(WQ, far_own, SIB_Q + 6, d_sib)
    recv(far_part, Q_RP)
    gather(WQ, far_part, SIB_Q + 7, d_sib)

    loads[5].wait()
    for i in range(8):
        recv(mine_o, SIB_O + i)

    def grad_cols(n, carry):
        rhs = WO[pl.ds(2 * n, 2)].reshape(256, D)
        AGR[:, pl.ds(pl.multiple_of(n * 256, 256), 256)] = dot(G[b_slot], rhs, 1, 1).astype(BF)
        return carry

    lax.fori_loop(0, 4, grad_cols, 0)
    loads[4].wait()
    for i in range(8):
        recv(mine_q, SIB_Q + i)

    lane = lax.broadcasted_iota(jnp.int32, (SEQ, 128), 1)
    first_half = lane % 64 < 32
    low = lane < 64

    def rot(u):
        return jnp.where(first_half, pltpu.roll(u, 96, 1), pltpu.roll(u, 32, 1))

    def rope(u):
        return u * cos_ref[...] + rot(u) * sin_ref[...]

    def unrope(u):
        return u * cos_ref[...] - rot(u) * sin_ref[...]

    def qkv_tile(n):
        sl = pl.ds(pl.multiple_of(n * 256, 256), 256)
        return dot(N[...], WQ[:, :, sl].reshape(D, 256), 1, 0)

    def q_cols(n, carry):
        t = qkv_tile(n)
        for i in range(2):
            Q[2 * n + i] = rope(t[:, i * 128 : (i + 1) * 128]).astype(BF)
        return carry

    lax.fori_loop(0, 4, q_cols, 0)
    for n, dst in ((4, KD), (5, VD)):
        t = qkv_tile(n)
        for i in range(2):
            u = t[:, i * 128 : (i + 1) * 128]
            if n == 4:
                u = rope(u)
            r = pltpu.roll(u, 64, 1)
            dst[2 * i] = jnp.where(low, u, r).astype(BF)
            dst[2 * i + 1] = jnp.where(low, r, u).astype(BF)

    causal = lax.broadcasted_iota(jnp.int32, (SEQ, SEQ), 0) <= lax.broadcasted_iota(
        jnp.int32, (SEQ, SEQ), 1
    )

    def one_kv(kv, carry):
        kd, vd = KD[kv], VD[kv]
        DKD[...] = jnp.zeros_like(DKD)
        DVD[...] = jnp.zeros_like(DVD)

        def pair(i, carry):
            t = kv * 2 + i
            q2 = Q[t]
            g2 = AGR[:, pl.ds(pl.multiple_of(t * 128, 128), 128)]
            dqs = []
            for keep in (low, jnp.logical_not(low)):
                qm = jnp.where(keep, q2, jnp.zeros_like(q2))
                gm = jnp.where(keep, g2, jnp.zeros_like(g2))
                e = jnp.where(causal, jnp.exp(dot(kd, qm, 1, 1) * SCALE), 0.0)
                probs = e * (1.0 / jnp.sum(e, axis=0, keepdims=True))
                DVD[...] += dot(probs.astype(BF), gm, 1, 0)
                dp = dot(vd, gm, 1, 1)
                delta = jnp.sum(probs * dp, axis=0, keepdims=True)
                ds = (probs * (dp - delta) * SCALE).astype(BF)
                DKD[...] += dot(ds, qm, 1, 0)
                dqs.append(dot(ds, kd, 0, 0))
            dq = jnp.where(low, dqs[0], dqs[1])
            GP[:, pl.ds(pl.multiple_of(t * 128, 128), 128)] = unrope(dq).astype(BF)
            return carry

        lax.fori_loop(0, 2, pair, 0)
        dk = DKD[...]
        dk = unrope(dk + pltpu.roll(dk, 64, 1))
        dv = DVD[...]
        dv = dv + pltpu.roll(dv, 64, 1)
        even = kv % 2 == 0
        keep = jnp.logical_xor(low, jnp.logical_not(even))
        for base, val in ((QW, dk), (QW + 256, dv)):
            sl = pl.ds(pl.multiple_of(base + (kv // 2) * 128, 128), 128)
            GP[:, sl] = jnp.where(keep, val.astype(BF), GP[:, sl])
        return carry

    GP[:, QW:] = jnp.zeros((SEQ, 512), BF)
    lax.fori_loop(0, 2, one_kv, 0)

    def add_into(dst, other):
        dst[...] = (dst[...].astype(F32) + other.astype(F32)).astype(BF)

    recv(R1Q.at[0], R1_Q + 0)
    add_into(qs(DQ, 0, up, c), R1Q[0])
    recv(R1Q.at[1], R1_Q + 1)
    add_into(qs(DQ, 1, down, c), R1Q[1])
    send(qs(DQ, 0, up, c), R2Q.at[0, 0], R2_Q + 0, d_up)
    send(qs(DQ, 1, down, c), R2Q.at[1, 1], R2_Q + 3, d_down)
    send(os(DO, 1, up, c), R2O.at[0, 1], R2_O + 1, d_up)
    send(os(DO, 0, down, c), R2O.at[1, 0], R2_O + 2, d_down)

    lax.fori_loop(2, 4, one_kv, 0)

    recv(R1O.at[0], R1_O + 0)
    add_into(os(DO, 0, up, c), R1O[0])
    recv(R1O.at[1], R1_O + 1)
    add_into(os(DO, 1, down, c), R1O[1])
    send(os(DO, 0, up, c), R2O.at[0, 0], R2_O + 0, d_up)
    send(os(DO, 1, down, c), R2O.at[1, 1], R2_O + 3, d_down)

    DOT[...] = jnp.zeros_like(DOT)

    def normed_cols(j, carry):
        sl = pl.ds(pl.multiple_of(j * 256, 256), 256)
        u = dot(GP[...], WQ[j], 1, 1) * gain_ref[:, sl]
        U[:, sl] = u
        ux = u * X[b_slot, :, sl].astype(F32)
        DOT[...] += ux[:, :128] + ux[:, 128:]
        return carry

    lax.fori_loop(0, CHIPS, normed_cols, 0)

    def finish(r, carry):
        sl = pl.ds(pl.multiple_of(r * 16, 16), 16)
        inv = INV[sl, :][:, :1]
        mean = jnp.sum(DOT[sl, :], axis=-1, keepdims=True) * (1.0 / D)
        wide = X[b_slot, sl, :].astype(F32)
        res = G[b_slot, sl, :].astype(F32) + inv * U[sl, :] - wide * (inv * inv * inv * mean)
        OUT[sl, :] = res.astype(BF)
        return carry

    for k in range(3):
        lax.fori_loop(8 * k, 8 * k + 8, finish, 0)
        rows = pl.ds(128 * k, 128)
        send(OUT.at[rows], prev_hbm.at[rows], PERM + k, d_prev)

    for i in range(4):
        recv(R2Q.at[i // 2, i % 2], R2_Q + i)

    def total(D_, slicer, R2, xx):
        return (
            slicer(D_, xx, y, c)[...].astype(F32) + R2[0, xx].astype(F32) + R2[1, xx].astype(F32)
        )

    theirs = qs(DQ, ox, y, c)
    theirs[...] = total(DQ, qs, R2Q, ox).astype(BF)
    gq_ref[...] = total(DQ, qs, R2Q, xh)
    send(theirs, RXQ, RX_Q, d_x)
    for i in range(4):
        recv(R2O.at[i // 2, i % 2], R2_O + i)
    theirs = os(DO, ox, y, c)
    theirs[...] = total(DO, os, R2O, ox).astype(BF)
    go_ref[...] = total(DO, os, R2O, xh)
    send(theirs, RXO, RX_O, d_x)
    recv(RXQ, RX_Q)
    gq_ref[...] += RXQ[...].astype(F32)
    recv(RXO, RX_O)
    go_ref[...] += RXO[...].astype(F32)
    for k in range(3):
        recv(prev_hbm.at[pl.ds(128 * k, 128)], PERM + k)
    for cp in started:
        cp.wait_send()


def local(x, g, a, p, wq, wo, gain, b, w):
    cos, sin = rope_tables()
    any_ = pl.BlockSpec(memory_space=pl.ANY)
    vm = pl.BlockSpec(memory_space=pltpu.VMEM)
    sm = pl.BlockSpec(memory_space=pltpu.SMEM)
    V = pltpu.VMEM
    prev, gq, go = pl.pallas_call(
        kernel,
        name="step",
        out_shape=(
            jax.ShapeDtypeStruct((SEQ, D), BF),
            jax.ShapeDtypeStruct((128, QKVW), F32),
            jax.ShapeDtypeStruct((64, D), F32),
        ),
        in_specs=[any_] * 6 + [vm, sm, sm, vm, vm],
        out_specs=(any_, vm, vm),
        scratch_shapes=[
            V((2, SEQ, D), BF), V((2, SEQ, D), BF), V((2, SEQ, QW), BF), V((2, SEQ, QKVW), BF),
            V((CHIPS, 256, QKVW), BF), V((CHIPS, 128, D), BF),
            V((CHIPS, 256, QKVW), BF), V((CHIPS, 128, D), BF),
            V((CHIPS, 128, QKVW), BF), V((CHIPS, 64, D), BF),
            V((2, 128, QKVW), BF), V((2, 64, D), BF),
            V((2, 2, 128, QKVW), BF), V((2, 2, 64, D), BF),
            V((128, QKVW), BF), V((64, D), BF),
            V((SEQ, D), BF), V((SEQ, 128), F32), V((8, SEQ, 128), BF),
            V((KV_HEADS, SEQ, 128), BF), V((KV_HEADS, SEQ, 128), BF),
            V((SEQ, QW), BF), V((SEQ, QKVW), BF), V((SEQ, 128), F32), V((SEQ, 128), F32),
            V((SEQ, D), F32), V((SEQ, 128), F32), V((SEQ, D), BF),
            pltpu.SemaphoreType.DMA((6,)),
            pltpu.SemaphoreType.DMA((N_SEM,)),
            pltpu.SemaphoreType.DMA((N_SEM,)),
        ],
        compiler_params=pltpu.CompilerParams(
            collective_id=0, has_side_effects=True, vmem_limit_bytes=67043328
        ),
    )(
        x[0], g[0], a[0], p[0], wq[0], wo[0], gain, b, w, jnp.asarray(cos), jnp.asarray(sin)
    )
    return prev[None], gq[None], go[None]


def solution(mesh):
    row = P("section", None, "fsdp", None)
    out = P("section", "fsdp", None)
    return jax.shard_map(
        local,
        mesh=mesh,
        in_specs=(row, row, row, row, out, out, P("section", None), P("section"), P("section")),
        out_specs=(out, out, out),
        check_vma=False,
    )
```

```python
import functools

import jax
import jax.numpy as jnp
import numpy as np
from jax import lax
from jax.experimental import pallas as pl
from jax.experimental.pallas import tpu as pltpu
from jax.sharding import PartitionSpec as P

D = 2048
HEAD_DIM = 64
HEADS = 16
KV_HEADS = 4
SEQ = 384
QW = 1024
QKVW = 1536
CHIPS = 8
EPS = 1e-05
SCALE = HEAD_DIM ** (-0.5)
BF = jnp.bfloat16
F32 = jnp.float32
MESH = pl.DeviceIdType.MESH

Q_X, Q_YP, Q_YM, Q_PP, Q_PM, Q_RO, Q_RP = range(7)
O_YP, O_YM, O_X0, O_XP, O_XM, O_X2, O_RA, O_RB = range(7, 15)
SIB_Q = 15
SIB_O = 23
RS_SIB_Q, RS_SIB_O = 31, 32
R1_Q, R1_O = 33, 35
R2_Q, R2_O = 37, 41
RX_Q, RX_O = 45, 46
PERM = 47
N_SEM = 50


def rope_tables():
    half = HEAD_DIM // 2
    freq = 500000.0 ** (-2.0 * np.arange(half) / HEAD_DIM)
    ang = np.arange(SEQ)[:, None] * freq[None, :]
    cos = np.tile(np.cos(ang), (1, 4)).astype(np.float32)
    sin = np.tile(np.sin(ang), (1, 4)).astype(np.float32)
    sign = np.where(np.arange(128) % 64 < 32, -1.0, 1.0).astype(np.float32)
    return cos, sin * sign[None, :]


def dot(a, b, ca, cb):
    return lax.dot_general(a, b, (((ca,), (cb,)), ((), ())), preferred_element_type=F32)


def kernel(
    x_hbm, g_hbm, a_hbm, p_hbm, wq_hbm, wo_hbm, gain_ref, b_ref, w_ref, cos_ref, sin_ref,
    prev_hbm, gq_ref, go_ref,
    X, G, A, PG, WQ, WO, DQ, DO, SQ, SO, R1Q, R1O, R2Q, R2O, RXQ, RXO,
    N, INV, QKV, QS, GS, KD, VD, GP, DK, DV, U, DOT, OUT,
    lsem, ssem, rsem,
):
    s = lax.axis_index("section")
    f = lax.axis_index("fsdp")
    xh, y, c = f // 8, (f // 2) % 4, f % 2
    up, down, far = (y + 1) % 4, (y + 3) % 4, (y + 2) % 4
    oc, ox = 1 - c, 1 - xh
    n_sec = lax.axis_size("section")

    def dev(xx, yy, cc):
        return (s, xx * 8 + yy * 2 + cc)

    d_up, d_down, d_x, d_sib = dev(xh, up, c), dev(xh, down, c), dev(ox, y, c), dev(xh, y, oc)
    d_prev, d_next = (lax.rem(s + n_sec - 1, n_sec), f), (lax.rem(s + 1, n_sec), f)

    def qs(ref, xx, yy, cc):
        return ref.at[xx * 4 + yy, pl.ds(pl.multiple_of(cc * 128, 128), 128), :]

    def os(ref, xx, yy, cc, lo=0, n=64):
        return ref.at[xx * 4 + yy, pl.ds(pl.multiple_of(cc * 64 + lo, 32), n), :]

    started = []
    scope = []

    def phase(name):
        if scope:
            scope.pop().__exit__(None, None, None)
        if name:
            scope.append(jax.named_scope(name))
            scope[-1].__enter__()

    def rcopy(src, dst, slot, device):
        return pltpu.make_async_remote_copy(
            src_ref=src, dst_ref=dst, send_sem=ssem.at[slot], recv_sem=rsem.at[slot],
            device_id=device, device_id_type=MESH,
        )

    def send(src, dst, slot, device):
        cp = rcopy(src, dst, slot, device)
        cp.start()
        started.append(cp)

    def recv(dst, slot):
        rcopy(dst, dst, slot, d_sib).wait_recv()

    def gather(ref, shard, slot, device, src=None):
        send(shard if src is None else src, shard, slot, device)

    phase("entry")
    barrier = pltpu.get_barrier_semaphore()
    for d in (d_up, d_down, d_x, d_sib, d_prev, d_next):
        pl.semaphore_signal(barrier, inc=1, device_id=d, device_id_type=MESH)
    loads = [
        pltpu.make_async_copy(g_hbm, G, lsem.at[0]),
        pltpu.make_async_copy(a_hbm, A, lsem.at[1]),
        pltpu.make_async_copy(x_hbm, X, lsem.at[2]),
        pltpu.make_async_copy(p_hbm, PG, lsem.at[3]),
        pltpu.make_async_copy(wq_hbm, qs(WQ, xh, y, c), lsem.at[4]),
        pltpu.make_async_copy(wo_hbm, os(WO, xh, y, c), lsem.at[5]),
    ]
    for cp in (loads[4], loads[5], loads[0], loads[1], loads[2], loads[3]):
        cp.start()
    pl.semaphore_wait(barrier, 6)

    phase("own_out")
    mine_q, mine_o = qs(WQ, xh, y, c), os(WO, xh, y, c)
    gather(WQ, mine_q, Q_X, d_x, wq_hbm)
    gather(WQ, mine_q, Q_YP, d_up, wq_hbm)
    gather(WQ, mine_q, Q_YM, d_down, wq_hbm)
    gather(WO, mine_o, O_YP, d_up, wo_hbm)
    gather(WO, mine_o, O_YM, d_down, wo_hbm)
    gather(WO, mine_o, O_X0, d_x, wo_hbm)
    gather(WQ, mine_q, SIB_Q + 0, d_sib, wq_hbm)
    gather(WO, mine_o, SIB_O + 0, d_sib, wo_hbm)

    b_slot, w_slot = b_ref[0], w_ref[0]

    phase("dw_out")
    loads[0].wait()
    loads[1].wait()

    def out_part(j, carry):
        lhs = A[w_slot, :, pl.ds(pl.multiple_of(j * 256, 256), 256)]
        part = dot(lhs, G[w_slot], 0, 0).astype(BF)
        DO[pl.ds(2 * j, 2)] = part.reshape(2, 128, D)
        return carry

    lax.fori_loop(0, 4, out_part, 0)
    send(DO.at[:, pl.ds(pl.multiple_of(oc * 64, 64), 64), :], SO, RS_SIB_O, d_sib)
    phase("norm_w")
    loads[2].wait()
    loads[3].wait()

    def norm(slot):
        def rows(r, carry):
            sl = pl.ds(pl.multiple_of(r * 16, 16), 16)
            wide = X[slot, sl, :].astype(F32)
            inv = lax.rsqrt(jnp.mean(wide * wide, axis=-1, keepdims=True) + EPS)
            INV[sl, :] = jnp.broadcast_to(inv, (16, 128))
            N[sl, :] = (wide * inv * gain_ref[...]).astype(BF)
            return carry

        lax.fori_loop(0, SEQ // 16, rows, 0, unroll=4)

    norm(w_slot)

    phase("dw_qkv")

    def qkv_part(j, carry):
        lhs = N[:, pl.ds(pl.multiple_of(j * 256, 256), 256)]
        DQ[j] = dot(lhs, PG[w_slot], 0, 0).astype(BF)
        return carry

    lax.fori_loop(0, CHIPS, qkv_part, 0)
    send(DQ.at[:, pl.ds(pl.multiple_of(oc * 128, 128), 128), :], SQ, RS_SIB_Q, d_sib)
    phase("norm_b")
    norm(b_slot)

    lane = lax.broadcasted_iota(jnp.int32, (128, 128), 1)
    first_half = lane % 64 < 32
    low = lane < 64

    def acc_qkv(xx, yy, first=False):
        j = xx * 4 + yy
        part = dot(N[:, pl.ds(pl.multiple_of(j * 256, 256), 256)], WQ[j], 1, 0)
        QKV[...] = part if first else QKV[...] + part

    def stack(ref, qb, kv, i, tile):
        zero = jnp.zeros_like(tile)
        ref[qb, kv, pl.ds(pl.multiple_of(i * 256, 256), 128)] = jnp.where(low, tile, zero)
        ref[qb, kv, pl.ds(pl.multiple_of(i * 256 + 128, 128), 128)] = jnp.where(low, zero, tile)

    def attn_grad(xx, yy):
        j = xx * 4 + yy
        tile = dot(G[b_slot], WO[j], 1, 1).astype(BF)
        for qb in range(3):
            stack(GS, qb, j // 2, j % 2, tile[qb * 128 : (qb + 1) * 128])

    def pair_sum_o(j, carry):
        so = pl.ds(pl.multiple_of(c * 64, 64), 64)
        DO[j, so, :] = (DO[j, so, :].astype(F32) + SO[j].astype(F32)).astype(BF)
        return carry

    def pair_sum_q(j, carry):
        sq = pl.ds(pl.multiple_of(c * 128, 128), 128)
        DQ[j, sq, :] = (DQ[j, sq, :].astype(F32) + SQ[j].astype(F32)).astype(BF)
        return carry

    sgn = 1 - 2 * xh
    ya, yb = (y + 4 - sgn) % 4, (y + 4 + sgn) % 4
    phase("fwd_xq")
    part_q = qs(WQ, ox, y, c)
    recv(part_q, Q_X)
    gather(WQ, part_q, Q_PP, d_up)
    gather(WQ, part_q, Q_PM, d_down)
    gather(WQ, part_q, SIB_Q + 1, d_sib)
    phase("fwd_yq")
    from_down, from_up = qs(WQ, xh, down, c), qs(WQ, xh, up, c)
    recv(from_down, Q_YP)
    recv(from_up, Q_YM)
    gather(WQ, from_down, SIB_Q + 2, d_sib)
    gather(WQ, from_up, SIB_Q + 3, d_sib)
    phase("sum_o")
    recv(SO, RS_SIB_O)
    lax.fori_loop(0, CHIPS, pair_sum_o, 0)
    phase("qkv_0")
    loads[4].wait()
    recv(mine_q, SIB_Q + 0)
    acc_qkv(xh, y, first=True)
    recv(mine_q, SIB_Q + 1)
    acc_qkv(ox, y)
    phase("fwd_yo")
    o_down, o_up = os(WO, xh, down, c), os(WO, xh, up, c)
    recv(o_down, O_YP)
    recv(o_up, O_YM)
    gather(WO, os(WO, xh, down, c, 0, 32), O_RA, d_up)
    gather(WO, os(WO, xh, up, c, 32, 32), O_RB, d_down)
    gather(WO, o_down, O_XP, d_x)
    gather(WO, o_up, O_XM, d_x)
    gather(WQ, qs(WQ, xh, ya, c), Q_RO, dev(xh, yb, c))
    gather(WO, o_down, SIB_O + 1, d_sib)
    gather(WO, o_up, SIB_O + 2, d_sib)
    o_part = os(WO, ox, y, c)
    recv(o_part, O_X0)
    gather(WO, o_part, SIB_O + 4, d_sib)
    phase("sum_q")
    recv(SQ, RS_SIB_Q)
    lax.fori_loop(0, CHIPS, pair_sum_q, 0)
    phase("qkv_1")
    recv(mine_q, SIB_Q + 2)
    acc_qkv(xh, down)
    recv(mine_q, SIB_Q + 3)
    acc_qkv(xh, up)
    phase("ag_0")
    loads[5].wait()
    recv(mine_o, SIB_O + 0)
    attn_grad(xh, y)
    recv(mine_o, SIB_O + 1)
    attn_grad(xh, down)

    phase("fwd_yp")
    part_down, part_up = qs(WQ, ox, down, c), qs(WQ, ox, up, c)
    recv(part_down, Q_PP)
    recv(part_up, Q_PM)
    gather(WQ, qs(WQ, ox, yb, c), Q_RP, dev(xh, ya, c))
    gather(WQ, part_down, SIB_Q + 4, d_sib)
    gather(WQ, part_up, SIB_Q + 5, d_sib)

    send(qs(DQ, 0, far, c), R1Q.at[0], R1_Q + 0, d_up)
    send(qs(DQ, 1, far, c), R1Q.at[1], R1_Q + 1, d_down)
    send(os(DO, 0, far, c), R1O.at[0], R1_O + 0, d_up)
    send(os(DO, 1, far, c), R1O.at[1], R1_O + 1, d_down)
    send(qs(DQ, 1, up, c), R2Q.at[0, 1], R2_Q + 1, d_up)
    send(qs(DQ, 0, down, c), R2Q.at[1, 0], R2_Q + 2, d_down)

    phase("fwd_ofar")
    o_far = os(WO, xh, far, c)
    recv(os(WO, xh, far, c, 0, 32), O_RA)
    recv(os(WO, xh, far, c, 32, 32), O_RB)
    gather(WO, o_far, O_X2, d_x)
    gather(WO, o_far, SIB_O + 3, d_sib)

    def pass_o(yy, slot, i):
        piece = os(WO, ox, yy, c)
        recv(piece, slot)
        gather(WO, piece, SIB_O + i, d_sib)

    pass_o(down, O_XP, 5)
    phase("ag_1")
    recv(mine_o, SIB_O + 2)
    attn_grad(xh, up)
    recv(mine_o, SIB_O + 4)
    attn_grad(ox, y)
    phase("fwd_xo")
    pass_o(up, O_XM, 6)
    phase("qkv_2")
    recv(mine_q, SIB_Q + 4)
    acc_qkv(ox, down)
    recv(mine_q, SIB_Q + 5)
    acc_qkv(ox, up)
    phase("ag_2")
    recv(mine_o, SIB_O + 5)
    attn_grad(ox, down)
    recv(mine_o, SIB_O + 3)
    attn_grad(xh, far)
    phase("fwd_qfar")
    far_own, far_part = qs(WQ, xh, far, c), qs(WQ, ox, far, c)
    recv(far_own, Q_RO)
    gather(WQ, far_own, SIB_Q + 6, d_sib)
    pass_o(far, O_X2, 7)
    recv(far_part, Q_RP)
    gather(WQ, far_part, SIB_Q + 7, d_sib)
    phase("ag_3")
    recv(mine_o, SIB_O + 6)
    attn_grad(ox, up)
    recv(mine_o, SIB_O + 7)
    attn_grad(ox, far)
    phase("qkv_3")
    recv(mine_q, SIB_Q + 6)
    acc_qkv(xh, far)
    recv(mine_q, SIB_Q + 7)
    acc_qkv(ox, far)

    phase("rope")

    def rot(u):
        return jnp.where(first_half, pltpu.roll(u, 96, 1), pltpu.roll(u, 32, 1))

    def rope(u, rows):
        return u * cos_ref[rows, :] + rot(u) * sin_ref[rows, :]

    def unrope(u, rows):
        return u * cos_ref[rows, :] - rot(u) * sin_ref[rows, :]

    for qb in range(3):
        rows = pl.ds(qb * 128, 128)

        def q_tile(t, carry):
            u = QKV[rows, pl.ds(pl.multiple_of(t * 128, 128), 128)]
            stack(QS, qb, t // 2, t % 2, rope(u, rows).astype(BF))
            return carry

        lax.fori_loop(0, 8, q_tile, 0, unroll=2)
        for base, dst in ((QW, KD), (QW + 256, VD)):
            for i in range(2):
                u = QKV[rows, base + i * 128 : base + (i + 1) * 128]
                if dst is KD:
                    u = rope(u, rows)
                r = pltpu.roll(u, 64, 1)
                dst[2 * i, rows, :] = jnp.where(low, u, r).astype(BF)
                dst[2 * i + 1, rows, :] = jnp.where(low, r, u).astype(BF)

    diag = lax.broadcasted_iota(jnp.int32, (128, 512), 0) <= (
        lax.broadcasted_iota(jnp.int32, (128, 512), 1) % 128
    )
    exp_scale = SCALE * 1.4426950408889634

    def attend(qb):
        keys = 128 * (qb + 1)
        rows = pl.ds(qb * 128, 128)

        def one_kv(kv, carry):
            kd, vd = KD[kv, :keys], VD[kv, :keys]
            q4, g4 = QS[qb, kv], GS[qb, kv]
            e = jnp.exp2(dot(kd, q4, 1, 1) * exp_scale)
            last = jnp.where(diag, e[keys - 128 :], 0.0)
            e = last if qb == 0 else jnp.concatenate([e[: keys - 128], last], axis=0)
            probs = e * (1.0 / jnp.sum(e, axis=0, keepdims=True))
            dv = dot(probs.astype(BF), g4, 1, 0)
            dp = dot(vd, g4, 1, 1)
            delta = jnp.sum(probs * dp, axis=0, keepdims=True)
            ds = (probs * (dp - delta)).astype(BF)
            dk = dot(ds, q4, 1, 0) * SCALE
            dq = dot(ds, kd, 0, 0) * SCALE
            if qb == 2:
                DK[kv], DV[kv] = dk, dv
            else:
                DK[kv, :keys] += dk
                DV[kv, :keys] += dv
            for i in range(2):
                tile = jnp.where(low, dq[256 * i : 256 * i + 128], dq[256 * i + 128 : 256 * i + 256])
                sl = pl.ds(pl.multiple_of((2 * kv + i) * 128, 128), 128)
                GP[:, sl] = unrope(tile, rows).astype(BF)
            return carry

        lax.fori_loop(0, KV_HEADS, one_kv, 0)
        for i in range(2):
            for base, ref in ((QW, DK), (QW + 256, DV)):
                halves = []
                for kv in (2 * i, 2 * i + 1):
                    t = ref[kv, rows]
                    halves.append(t + pltpu.roll(t, 64, 1))
                tile = jnp.where(low, halves[0], halves[1])
                if ref is DK:
                    tile = unrope(tile, rows)
                GP[:, base + i * 128 : base + (i + 1) * 128] = tile.astype(BF)

    def input_grad(qb):
        rows = pl.ds(qb * 128, 128)
        DOT[...] = jnp.zeros_like(DOT)

        def normed_cols(j, carry):
            sl = pl.ds(pl.multiple_of(j * 256, 256), 256)
            u = dot(GP[...], WQ[j], 1, 1) * gain_ref[:, sl]
            U[:, sl] = u
            ux = u * X[b_slot, rows, sl].astype(F32)
            DOT[...] += ux[:, :128] + ux[:, 128:]
            return carry

        lax.fori_loop(0, CHIPS, normed_cols, 0, unroll=2)
        inv = INV[rows, :]
        mean = jnp.sum(DOT[...], axis=-1, keepdims=True) * (1.0 / D)
        DOT[...] = inv * inv * inv * mean

        def finish(j, carry):
            for r in range(4):
                part = pl.ds(32 * r, 32)
                here = pl.ds(qb * 128 + 32 * r, 32)
                sl = pl.ds(pl.multiple_of(j * 128, 128), 128)
                res = (
                    G[b_slot, here, sl].astype(F32)
                    + INV[here, :] * U[part, sl]
                    - X[b_slot, here, sl].astype(F32) * DOT[part, :]
                )
                OUT[here, sl] = res.astype(BF)
            return carry

        lax.fori_loop(0, 16, finish, 0, unroll=2)
        send(OUT.at[rows], prev_hbm.at[rows], PERM + qb, d_prev)

    def add_into(dst, other):
        dst[...] = (dst[...].astype(F32) + other.astype(F32)).astype(BF)

    phase("attn_2")
    attend(2)
    phase("ig_2")
    input_grad(2)

    phase("rs_relay_q")
    recv(R1Q.at[0], R1_Q + 0)
    add_into(qs(DQ, 0, up, c), R1Q[0])
    recv(R1Q.at[1], R1_Q + 1)
    add_into(qs(DQ, 1, down, c), R1Q[1])
    send(qs(DQ, 0, up, c), R2Q.at[0, 0], R2_Q + 0, d_up)
    send(qs(DQ, 1, down, c), R2Q.at[1, 1], R2_Q + 3, d_down)
    send(os(DO, 1, up, c), R2O.at[0, 1], R2_O + 1, d_up)
    send(os(DO, 0, down, c), R2O.at[1, 0], R2_O + 2, d_down)
    phase("attn_1")
    attend(1)
    phase("ig_1")
    input_grad(1)
    phase("rs_relay_o")
    recv(R1O.at[0], R1_O + 0)
    add_into(os(DO, 0, up, c), R1O[0])
    recv(R1O.at[1], R1_O + 1)
    add_into(os(DO, 1, down, c), R1O[1])
    send(os(DO, 0, up, c), R2O.at[0, 0], R2_O + 0, d_up)
    send(os(DO, 1, down, c), R2O.at[1, 1], R2_O + 3, d_down)
    phase("attn_0")
    attend(0)
    phase("ig_0")
    input_grad(0)

    phase("rs_wait_q")
    for i in range(4):
        recv(R2Q.at[i // 2, i % 2], R2_Q + i)

    phase("rs_tot_q")
    def total(D_, slicer, R2, xx):
        return (
            slicer(D_, xx, y, c)[...].astype(F32) + R2[0, xx].astype(F32) + R2[1, xx].astype(F32)
        )

    theirs = qs(DQ, ox, y, c)
    theirs[...] = total(DQ, qs, R2Q, ox).astype(BF)
    gq_ref[...] = total(DQ, qs, R2Q, xh)
    send(theirs, RXQ, RX_Q, d_x)
    phase("rs_wait_o")
    for i in range(4):
        recv(R2O.at[i // 2, i % 2], R2_O + i)
    theirs = os(DO, ox, y, c)
    theirs[...] = total(DO, os, R2O, ox).astype(BF)
    go_ref[...] = total(DO, os, R2O, xh)
    send(theirs, RXO, RX_O, d_x)
    phase("rs_x_wait")
    recv(RXQ, RX_Q)
    gq_ref[...] += RXQ[...].astype(F32)
    recv(RXO, RX_O)
    go_ref[...] += RXO[...].astype(F32)
    phase("perm_wait")
    for k in range(3):
        recv(prev_hbm.at[pl.ds(128 * k, 128)], PERM + k)
    phase("send_wait")
    for cp in started:
        cp.wait_send()
    phase(None)


def local(x, g, a, p, wq, wo, gain, b, w):
    cos, sin = rope_tables()
    any_ = pl.BlockSpec(memory_space=pl.ANY)
    vm = pl.BlockSpec(memory_space=pltpu.VMEM)
    sm = pl.BlockSpec(memory_space=pltpu.SMEM)
    V = pltpu.VMEM
    prev, gq, go = pl.pallas_call(
        kernel,
        name="step",
        out_shape=(
            jax.ShapeDtypeStruct((SEQ, D), BF),
            jax.ShapeDtypeStruct((128, QKVW), F32),
            jax.ShapeDtypeStruct((64, D), F32),
        ),
        in_specs=[any_] * 6 + [vm, sm, sm, vm, vm],
        out_specs=(any_, vm, vm),
        scratch_shapes=[
            V((2, SEQ, D), BF), V((2, SEQ, D), BF), V((2, SEQ, QW), BF), V((2, SEQ, QKVW), BF),
            V((CHIPS, 256, QKVW), BF), V((CHIPS, 128, D), BF),
            V((CHIPS, 256, QKVW), BF), V((CHIPS, 128, D), BF),
            V((CHIPS, 128, QKVW), BF), V((CHIPS, 64, D), BF),
            V((2, 128, QKVW), BF), V((2, 64, D), BF),
            V((2, 2, 128, QKVW), BF), V((2, 2, 64, D), BF),
            V((128, QKVW), BF), V((64, D), BF),
            V((SEQ, D), BF), V((SEQ, 128), F32), V((SEQ, QKVW), F32),
            V((3, KV_HEADS, 512, 128), BF), V((3, KV_HEADS, 512, 128), BF),
            V((KV_HEADS, SEQ, 128), BF), V((KV_HEADS, SEQ, 128), BF),
            V((128, QKVW), BF), V((KV_HEADS, SEQ, 128), F32), V((KV_HEADS, SEQ, 128), F32),
            V((128, D), F32), V((128, 128), F32), V((SEQ, D), BF),
            pltpu.SemaphoreType.DMA((6,)),
            pltpu.SemaphoreType.DMA((N_SEM,)),
            pltpu.SemaphoreType.DMA((N_SEM,)),
        ],
        compiler_params=pltpu.CompilerParams(
            collective_id=0, has_side_effects=True, vmem_limit_bytes=67043328
        ),
    )(
        x[0], g[0], a[0], p[0], wq[0], wo[0], gain, b, w, jnp.asarray(cos), jnp.asarray(sin)
    )
    return prev[None], gq[None], go[None]


def solution(mesh):
    row = P("section", None, "fsdp", None)
    out = P("section", "fsdp", None)
    return jax.shard_map(
        local,
        mesh=mesh,
        in_specs=(row, row, row, row, out, out, P("section", None), P("section"), P("section")),
        out_specs=(out, out, out),
        check_vma=False,
    )
```

```python
import functools

import jax
import jax.numpy as jnp
import numpy as np
from jax import lax
from jax.experimental import pallas as pl
from jax.experimental.pallas import tpu as pltpu
from jax.sharding import PartitionSpec as P

D = 2048
HEAD_DIM = 64
HEADS = 16
KV_HEADS = 4
SEQ = 384
QW = 1024
QKVW = 1536
CHIPS = 8
EPS = 1e-05
SCALE = HEAD_DIM ** (-0.5)
BF = jnp.bfloat16
F32 = jnp.float32
MESH = pl.DeviceIdType.MESH

Q_X, Q_YP, Q_YM, Q_PP, Q_PM, Q_RO, Q_RP = range(7)
O_YP, O_YM, O_X0, O_XP, O_XM, O_X2, O_RA, O_RB = range(7, 15)
SIB_Q = 15
SIB_O = 23
RS_SIB_Q, RS_SIB_O = 31, 32
R1_Q, R1_O = 33, 35
R2_Q, R2_O = 37, 41
RX_Q, RX_O = 45, 46
PERM = 47
Q_PP2, Q_PM2, Q_RP2 = 51, 52, 53
XB_S = 54
R1_B = 55
R2_B = 57
N_SEM = 61
XROWS = 16
LOW = 64 - XROWS


def rope_tables():
    half = HEAD_DIM // 2
    freq = 500000.0 ** (-2.0 * np.arange(half) / HEAD_DIM)
    ang = np.arange(SEQ)[:, None] * freq[None, :]
    cos = np.tile(np.cos(ang), (1, 4)).astype(np.float32)
    sin = np.tile(np.sin(ang), (1, 4)).astype(np.float32)
    sign = np.where(np.arange(128) % 64 < 32, -1.0, 1.0).astype(np.float32)
    return cos, sin * sign[None, :]


def dot(a, b, ca, cb):
    return lax.dot_general(a, b, (((ca,), (cb,)), ((), ())), preferred_element_type=F32)


def kernel(
    x_hbm, g_hbm, a_hbm, p_hbm, wq_hbm, wo_hbm, gain_hbm, b_hbm, w_hbm, cos_hbm, sin_hbm,
    prev_ref, gq_ref, go_ref,
    X, G, A, PG, WQ, WO, DQ, DO, SQ, SO, R1Q, R1O, R2Q, R2O, RXQ, RXO, XB, R1B, R2B,
    N, INV, QKV, QS, GS, KD, VD, GP, DK, DV, U, DOT, OUT,
    gain_ref, cos_ref, sin_ref, b_ref, w_ref,
    lsem, ssem, rsem, ready,
):
    s = lax.axis_index("section")
    f = lax.axis_index("fsdp")
    xh, y, c = f // 8, (f // 2) % 4, f % 2
    up, down, far = (y + 1) % 4, (y + 3) % 4, (y + 2) % 4
    oc, ox = 1 - c, 1 - xh
    n_sec = lax.axis_size("section")

    def dev(xx, yy, cc):
        return (s, xx * 8 + yy * 2 + cc)

    d_up, d_down, d_x, d_sib = dev(xh, up, c), dev(xh, down, c), dev(ox, y, c), dev(xh, y, oc)
    d_prev, d_next = (lax.rem(s + n_sec - 1, n_sec), f), (lax.rem(s + 1, n_sec), f)

    def qs(ref, xx, yy, cc, lo=0, n=128):
        return ref.at[xx * 4 + yy, pl.ds(pl.multiple_of(cc * 128 + lo, 64), n), :]

    def os(ref, xx, yy, cc, lo=0, n=64):
        return ref.at[xx * 4 + yy, pl.ds(pl.multiple_of(cc * 64 + lo, 16), n), :]

    started = []
    scope = []

    def phase(name):
        if scope:
            scope.pop().__exit__(None, None, None)
        if name:
            scope.append(jax.named_scope(name))
            scope[-1].__enter__()

    def rcopy(src, dst, slot, device):
        return pltpu.make_async_remote_copy(
            src_ref=src, dst_ref=dst, send_sem=ssem.at[slot], recv_sem=rsem.at[slot],
            device_id=device, device_id_type=MESH,
        )

    def send(src, dst, slot, device):
        cp = rcopy(src, dst, slot, device)
        cp.start()
        started.append(cp)

    def recv(dst, slot):
        rcopy(dst, dst, slot, d_sib).wait_recv()

    def gather(ref, shard, slot, device, src=None):
        send(shard if src is None else src, shard, slot, device)

    phase("entry")
    barrier = pltpu.get_barrier_semaphore()
    for d in (d_up, d_down, d_x, d_sib, d_prev):
        pl.semaphore_signal(barrier, inc=1, device_id=d, device_id_type=MESH)
    loads = [
        pltpu.make_async_copy(g_hbm, G, lsem.at[0]),
        pltpu.make_async_copy(a_hbm, A, lsem.at[1]),
        pltpu.make_async_copy(x_hbm, X, lsem.at[2]),
        pltpu.make_async_copy(p_hbm, PG, lsem.at[3]),
        pltpu.make_async_copy(wq_hbm, qs(WQ, xh, y, c), lsem.at[4]),
        pltpu.make_async_copy(wo_hbm, os(WO, xh, y, c), lsem.at[5]),
        pltpu.make_async_copy(gain_hbm, gain_ref, lsem.at[6]),
        pltpu.make_async_copy(cos_hbm, cos_ref, lsem.at[7]),
        pltpu.make_async_copy(sin_hbm, sin_ref, lsem.at[8]),
        pltpu.make_async_copy(b_hbm, b_ref, lsem.at[9]),
        pltpu.make_async_copy(w_hbm, w_ref, lsem.at[10]),
    ]
    for i in (9, 10, 4, 5, 0, 1, 6, 2, 3, 7, 8):
        cp = loads[i]
        cp.start()
    pl.semaphore_wait(barrier, 5)
    pl.semaphore_signal(ready, inc=1, device_id=d_next, device_id_type=MESH)

    phase("own_out")
    mine_q, mine_o = qs(WQ, xh, y, c), os(WO, xh, y, c)
    gather(WQ, mine_q, Q_X, d_x, wq_hbm)
    gather(WQ, mine_q, Q_YP, d_up, wq_hbm)
    gather(WQ, mine_q, Q_YM, d_down, wq_hbm)
    gather(WO, mine_o, O_YP, d_up, wo_hbm)
    gather(WO, mine_o, O_YM, d_down, wo_hbm)
    gather(WO, mine_o, O_X0, d_x, wo_hbm)
    gather(WQ, mine_q, SIB_Q + 0, d_sib, wq_hbm)
    gather(WO, mine_o, SIB_O + 0, d_sib, wo_hbm)

    loads[9].wait()
    loads[10].wait()
    b_slot, w_slot = b_ref[0], w_ref[0]

    phase("dw_out")
    loads[0].wait()
    loads[1].wait()

    def out_part(j, carry):
        lhs = A[w_slot, :, pl.ds(pl.multiple_of(j * 256, 256), 256)]
        part = dot(lhs, G[w_slot], 0, 0).astype(BF)
        DO[pl.ds(2 * j, 2)] = part.reshape(2, 128, D)
        return carry

    lax.fori_loop(0, 4, out_part, 0)
    send(DO.at[:, pl.ds(pl.multiple_of(oc * 64, 64), 64), :], SO, RS_SIB_O, d_sib)
    phase("norm_w")
    loads[2].wait()
    loads[3].wait()
    loads[6].wait()

    def norm(slot):
        def rows(r, carry):
            sl = pl.ds(pl.multiple_of(r * 16, 16), 16)
            wide = X[slot, sl, :].astype(F32)
            inv = lax.rsqrt(jnp.mean(wide * wide, axis=-1, keepdims=True) + EPS)
            INV[sl, :] = jnp.broadcast_to(inv, (16, 128))
            N[sl, :] = (wide * inv * gain_ref[...]).astype(BF)
            return carry

        lax.fori_loop(0, SEQ // 16, rows, 0, unroll=4)

    norm(w_slot)

    phase("dw_qkv")

    def qkv_part(j, carry):
        lhs = N[:, pl.ds(pl.multiple_of(j * 256, 256), 256)]
        DQ[j] = dot(lhs, PG[w_slot], 0, 0).astype(BF)
        return carry

    lax.fori_loop(0, CHIPS, qkv_part, 0)
    send(DQ.at[:, pl.ds(pl.multiple_of(oc * 128, 128), 128), :], SQ, RS_SIB_Q, d_sib)
    phase("norm_b")
    norm(b_slot)

    lane = lax.broadcasted_iota(jnp.int32, (128, 128), 1)
    first_half = lane % 64 < 32
    low = lane < 64

    def acc_qkv(xx, yy, first=False):
        j = xx * 4 + yy
        part = dot(N[:, pl.ds(pl.multiple_of(j * 256, 256), 256)], WQ[j], 1, 0)
        QKV[...] = part if first else QKV[...] + part

    def stack(ref, b, kv, i, tile):
        zero = jnp.zeros_like(tile)
        ref[kv, b, pl.ds(pl.multiple_of(i * 128, 128), 64)] = jnp.where(low[:64], tile, zero)
        ref[kv, b, pl.ds(pl.multiple_of(i * 128 + 64, 64), 64)] = jnp.where(low[:64], zero, tile)

    def attn_grad(xx, yy):
        j = xx * 4 + yy
        tile = dot(G[b_slot], WO[j], 1, 1).astype(BF)
        for b in range(6):
            stack(GS, b, j // 2, j % 2, tile[b * 64 : (b + 1) * 64])

    def pair_sum_o(j, carry):
        so = pl.ds(pl.multiple_of(c * 64, 64), 64)
        DO[j, so, :] = (DO[j, so, :].astype(F32) + SO[j].astype(F32)).astype(BF)
        return carry

    def pair_sum_q(j, carry):
        sq = pl.ds(pl.multiple_of(c * 128, 128), 128)
        DQ[j, sq, :] = (DQ[j, sq, :].astype(F32) + SQ[j].astype(F32)).astype(BF)
        return carry

    sgn = 1 - 2 * xh
    ya, yb = (y + 4 - sgn) % 4, (y + 4 + sgn) % 4
    phase("fwd_xq")
    part_q = qs(WQ, ox, y, c)
    recv(part_q, Q_X)
    gather(WQ, qs(WQ, ox, y, c, 0, 64), Q_PP, d_up)
    gather(WQ, qs(WQ, ox, y, c, 0, 64), Q_PM, d_down)
    gather(WQ, part_q, SIB_Q + 1, d_sib)
    phase("fwd_yq")
    from_down, from_up = qs(WQ, xh, down, c), qs(WQ, xh, up, c)
    recv(from_down, Q_YP)
    recv(from_up, Q_YM)
    gather(WQ, from_down, SIB_Q + 2, d_sib)
    gather(WQ, from_up, SIB_Q + 3, d_sib)
    phase("sum_o")
    recv(SO, RS_SIB_O)
    lax.fori_loop(0, CHIPS, pair_sum_o, 0)
    phase("qkv_0")
    loads[4].wait()
    recv(mine_q, SIB_Q + 0)
    acc_qkv(xh, y, first=True)
    recv(mine_q, SIB_Q + 1)
    acc_qkv(ox, y)
    phase("fwd_yo")
    o_down, o_up = os(WO, xh, down, c), os(WO, xh, up, c)
    recv(o_down, O_YP)
    recv(o_up, O_YM)
    gather(WO, os(WO, xh, down, c, 0, 32), O_RA, d_up)
    gather(WO, os(WO, xh, up, c, 32, 32), O_RB, d_down)
    gather(WQ, qs(WQ, ox, y, c, 64, 64), Q_PP2, d_up)
    gather(WQ, qs(WQ, ox, y, c, 64, 64), Q_PM2, d_down)
    gather(WO, o_down, O_XP, d_x)
    gather(WO, o_up, O_XM, d_x)
    gather(WQ, qs(WQ, xh, ya, c), Q_RO, dev(xh, yb, c))
    gather(WO, o_down, SIB_O + 1, d_sib)
    gather(WO, o_up, SIB_O + 2, d_sib)
    o_part = os(WO, ox, y, c)
    recv(o_part, O_X0)
    gather(WO, o_part, SIB_O + 4, d_sib)
    phase("qkv_1")
    recv(mine_q, SIB_Q + 2)
    acc_qkv(xh, down)
    recv(mine_q, SIB_Q + 3)
    acc_qkv(xh, up)
    phase("ag_0")
    loads[5].wait()
    recv(mine_o, SIB_O + 0)
    attn_grad(xh, y)
    recv(mine_o, SIB_O + 1)
    attn_grad(xh, down)
    recv(mine_o, SIB_O + 2)
    attn_grad(xh, up)
    recv(mine_o, SIB_O + 4)
    attn_grad(ox, y)

    phase("fwd_yp1")
    recv(qs(WQ, ox, down, c, 0, 64), Q_PP)
    recv(qs(WQ, ox, up, c, 0, 64), Q_PM)
    gather(WQ, qs(WQ, ox, yb, c, 0, 64), Q_RP, dev(xh, ya, c))
    phase("fwd_ofar")
    o_far = os(WO, xh, far, c)
    recv(os(WO, xh, far, c, 0, 32), O_RA)
    recv(os(WO, xh, far, c, 32, 32), O_RB)
    gather(WO, o_far, O_X2, d_x)
    gather(WO, o_far, SIB_O + 3, d_sib)
    phase("fwd_yp")
    part_down, part_up = qs(WQ, ox, down, c), qs(WQ, ox, up, c)
    recv(qs(WQ, ox, down, c, 64, 64), Q_PP2)
    recv(qs(WQ, ox, up, c, 64, 64), Q_PM2)
    gather(WQ, qs(WQ, ox, yb, c, 64, 64), Q_RP2, dev(xh, ya, c))
    gather(WQ, part_down, SIB_Q + 4, d_sib)
    gather(WQ, part_up, SIB_Q + 5, d_sib)

    def pass_o(yy, slot, i):
        piece = os(WO, ox, yy, c)
        recv(piece, slot)
        gather(WO, piece, SIB_O + i, d_sib)

    pass_o(down, O_XP, 5)
    phase("sum_q")
    recv(SQ, RS_SIB_Q)
    lax.fori_loop(0, CHIPS, pair_sum_q, 0)
    send(qs(DQ, 0, far, c), R1Q.at[0], R1_Q + 0, d_up)
    send(qs(DQ, 1, far, c), R1Q.at[1], R1_Q + 1, d_down)
    send(os(DO, 0, far, c, 0, LOW), R1O.at[0], R1_O + 0, d_up)
    send(os(DO, 1, far, c, 0, LOW), R1O.at[1], R1_O + 1, d_down)
    send(qs(DQ, 1, up, c), R2Q.at[0, 1], R2_Q + 1, d_up)
    send(qs(DQ, 0, down, c), R2Q.at[1, 0], R2_Q + 2, d_down)
    phase("ag_1")
    recv(mine_o, SIB_O + 5)
    attn_grad(ox, down)
    phase("qkv_2")
    recv(mine_q, SIB_Q + 4)
    acc_qkv(ox, down)
    recv(mine_q, SIB_Q + 5)
    acc_qkv(ox, up)
    phase("fwd_xo")
    pass_o(up, O_XM, 6)
    phase("ag_2")
    recv(mine_o, SIB_O + 3)
    attn_grad(xh, far)
    recv(mine_o, SIB_O + 6)
    attn_grad(ox, up)
    phase("fwd_qfar")
    pass_o(far, O_X2, 7)
    send(
        DO.at[pl.ds(ox * 4, 4), pl.ds(pl.multiple_of(c * 64 + LOW, 16), XROWS), :], XB, XB_S, d_x
    )
    far_own, far_part = qs(WQ, xh, far, c), qs(WQ, ox, far, c)
    recv(far_own, Q_RO)
    gather(WQ, far_own, SIB_Q + 6, d_sib)
    recv(qs(WQ, ox, far, c, 0, 64), Q_RP)
    recv(qs(WQ, ox, far, c, 64, 64), Q_RP2)
    gather(WQ, far_part, SIB_Q + 7, d_sib)
    phase("ag_3")
    recv(mine_o, SIB_O + 7)
    attn_grad(ox, far)
    phase("qkv_3")
    recv(mine_q, SIB_Q + 6)
    acc_qkv(xh, far)
    recv(mine_q, SIB_Q + 7)
    acc_qkv(ox, far)

    phase("rope")
    loads[7].wait()
    loads[8].wait()

    def rot(u):
        mask = first_half[: u.shape[0]]
        return jnp.where(mask, pltpu.roll(u, 96, 1), pltpu.roll(u, 32, 1))

    def rope(u, rows):
        return u * cos_ref[rows, :] + rot(u) * sin_ref[rows, :]

    def unrope(u, rows):
        return u * cos_ref[rows, :] - rot(u) * sin_ref[rows, :]

    def rope_q(b):
        rows = pl.ds(b * 64, 64)
        for t in range(8):
            u = QKV[rows, t * 128 : (t + 1) * 128]
            stack(QS, b, t // 2, t % 2, rope(u, rows).astype(BF))

    for qb in range(3):
        rows = pl.ds(qb * 128, 128)
        for base, dst in ((QW, KD), (QW + 256, VD)):
            for i in range(2):
                u = QKV[rows, base + i * 128 : base + (i + 1) * 128]
                if dst is KD:
                    u = rope(u, rows)
                r = pltpu.roll(u, 64, 1)
                dst[2 * i, rows, :] = jnp.where(low, u, r).astype(BF)
                dst[2 * i + 1, rows, :] = jnp.where(low, r, u).astype(BF)
    rope_q(5)

    exp_scale = SCALE * 1.4426950408889634

    def attend(b0, nb):
        n = nb * 64
        keys = b0 * 64 + n
        rows = pl.ds(b0 * 64, n)
        col = lax.broadcasted_iota(jnp.int32, (n, 4 * n), 1)
        diag = lax.broadcasted_iota(jnp.int32, (n, 4 * n), 0) <= (col // 256) * 64 + col % 64
        low_n = low[:n]

        def one_kv(kv, carry):
            kd, vd = KD[kv, :keys], VD[kv, :keys]
            q4 = QS[kv, b0 : b0 + nb].reshape(4 * n, 128)
            g4 = GS[kv, b0 : b0 + nb].reshape(4 * n, 128)
            e = jnp.exp2(dot(kd, q4, 1, 1) * exp_scale)
            last = jnp.where(diag, e[keys - n :], 0.0)
            e = last if b0 == 0 else jnp.concatenate([e[: keys - n], last], axis=0)
            probs = e * (1.0 / jnp.sum(e, axis=0, keepdims=True))
            dv = dot(probs.astype(BF), g4, 1, 0)
            dp = dot(vd, g4, 1, 1)
            delta = jnp.sum(probs * dp, axis=0, keepdims=True)
            ds = (probs * (dp - delta)).astype(BF)
            dk = dot(ds, q4, 1, 0) * SCALE
            dq = dot(ds, kd, 0, 0) * SCALE
            if keys == SEQ:
                DK[kv], DV[kv] = dk, dv
            else:
                DK[kv, :keys] += dk
                DV[kv, :keys] += dv
            for i in range(2):
                head = [
                    jnp.concatenate(
                        [dq[256 * k + 64 * h : 256 * k + 64 * h + 64] for k in range(nb)], axis=0
                    )
                    for h in (2 * i, 2 * i + 1)
                ]
                sl = pl.ds(pl.multiple_of((2 * kv + i) * 128, 128), 128)
                GP[:n, sl] = unrope(jnp.where(low_n, head[0], head[1]), rows).astype(BF)
            return carry

        lax.fori_loop(0, KV_HEADS, one_kv, 0, unroll=4)
        for i in range(2):
            for base, ref in ((QW, DK), (QW + 256, DV)):
                halves = []
                for kv in (2 * i, 2 * i + 1):
                    t = ref[kv, rows]
                    halves.append(t + pltpu.roll(t, 64, 1))
                tile = jnp.where(low_n, halves[0], halves[1])
                if ref is DK:
                    tile = unrope(tile, rows)
                GP[:n, base + i * 128 : base + (i + 1) * 128] = tile.astype(BF)

    def input_grad(b0, nb, slot):
        n = nb * 64
        rows = pl.ds(b0 * 64, n)
        DOT[...] = jnp.zeros_like(DOT)

        def normed_cols(j, carry):
            sl = pl.ds(pl.multiple_of(j * 256, 256), 256)
            u = dot(GP[:n], WQ[j], 1, 1) * gain_ref[:, sl]
            U[:n, sl] = u
            ux = u * X[b_slot, rows, sl].astype(F32)
            DOT[:n] += ux[:, :128] + ux[:, 128:]
            return carry

        lax.fori_loop(0, CHIPS, normed_cols, 0, unroll=2)
        phase(f"fin_{b0}")
        inv = INV[rows, :]
        mean = jnp.sum(DOT[:n], axis=-1, keepdims=True) * (1.0 / D)
        DOT[:n] = inv * inv * inv * mean

        def finish(j, carry):
            sl = pl.ds(pl.multiple_of(j * 128, 128), 128)
            for r in range(n // 32):
                part = pl.ds(32 * r, 32)
                here = pl.ds(b0 * 64 + 32 * r, 32)
                res = (
                    G[b_slot, here, sl].astype(F32)
                    + INV[here, :] * U[part, sl]
                    - X[b_slot, here, sl].astype(F32) * DOT[part, :]
                )
                OUT[here, sl] = res.astype(BF)
            return carry

        lax.fori_loop(0, 16, finish, 0, unroll=4)
        if slot == 0:
            pl.semaphore_wait(ready, 1)
        send(OUT.at[rows], prev_ref.at[rows], PERM + slot, d_prev)

    def add_into(dst, other):
        dst[...] = (dst[...].astype(F32) + other.astype(F32)).astype(BF)

    phase("attn_5")
    attend(5, 1)
    phase("ig_5")
    input_grad(5, 1, 0)
    phase("attn_4")
    rope_q(4)
    attend(4, 1)
    phase("ig_4")
    input_grad(4, 1, 1)

    phase("rs_relay_q")
    recv(R1Q.at[0], R1_Q + 0)
    add_into(qs(DQ, 0, up, c), R1Q[0])
    recv(R1Q.at[1], R1_Q + 1)
    add_into(qs(DQ, 1, down, c), R1Q[1])
    send(qs(DQ, 0, up, c), R2Q.at[0, 0], R2_Q + 0, d_up)
    send(qs(DQ, 1, down, c), R2Q.at[1, 1], R2_Q + 3, d_down)
    send(os(DO, 1, up, c, 0, LOW), R2O.at[0, 1], R2_O + 1, d_up)
    send(os(DO, 0, down, c, 0, LOW), R2O.at[1, 0], R2_O + 2, d_down)
    recv(XB, XB_S)
    for i in range(4):
        XB[i] = (XB[i].astype(F32) + os(DO, xh, i, c, LOW, XROWS)[...].astype(F32)).astype(BF)
    c0, c1 = pl.ds(0, D // 2), pl.ds(D // 2, D // 2)
    send(XB.at[far, :, c0], R1B.at[0], R1_B + 0, d_up)
    send(XB.at[far, :, c1], R1B.at[1], R1_B + 1, d_down)
    send(XB.at[up, :, c1], R2B.at[0, :, c1], R2_B + 1, d_up)
    send(XB.at[down, :, c0], R2B.at[1, :, c0], R2_B + 2, d_down)
    phase("attn_2")
    for b in range(4):
        rope_q(b)
    attend(2, 2)
    phase("ig_2")
    input_grad(2, 2, 2)
    phase("rs_relay_o")
    recv(R1O.at[0], R1_O + 0)
    add_into(os(DO, 0, up, c, 0, LOW), R1O[0])
    recv(R1O.at[1], R1_O + 1)
    add_into(os(DO, 1, down, c, 0, LOW), R1O[1])
    send(os(DO, 0, up, c, 0, LOW), R2O.at[0, 0], R2_O + 0, d_up)
    send(os(DO, 1, down, c, 0, LOW), R2O.at[1, 1], R2_O + 3, d_down)
    phase("attn_0")
    attend(0, 2)
    phase("ig_0")
    input_grad(0, 2, 3)

    phase("rs_wait_q")
    for i in range(4):
        recv(R2Q.at[i // 2, i % 2], R2_Q + i)
    phase("rs_tot_q")

    def total(mine, R2, xx):
        return mine[...].astype(F32) + R2[0, xx].astype(F32) + R2[1, xx].astype(F32)

    theirs = qs(DQ, ox, y, c)
    theirs[...] = total(theirs, R2Q, ox).astype(BF)
    gq_ref[...] = total(qs(DQ, xh, y, c), R2Q, xh)
    send(theirs, RXQ, RX_Q, d_x)
    phase("rs_relay_b")
    recv(R1B.at[0], R1_B + 0)
    add_into(XB.at[up, :, c0], R1B[0])
    recv(R1B.at[1], R1_B + 1)
    add_into(XB.at[down, :, c1], R1B[1])
    send(XB.at[up, :, c0], R2B.at[0, :, c0], R2_B + 0, d_up)
    send(XB.at[down, :, c1], R2B.at[1, :, c1], R2_B + 3, d_down)
    phase("rs_wait_o")
    for i in range(4):
        recv(R2O.at[i // 2, i % 2], R2_O + i)
    theirs = os(DO, ox, y, c, 0, LOW)
    theirs[...] = total(theirs, R2O, ox).astype(BF)
    go_ref[:LOW] = total(os(DO, xh, y, c, 0, LOW), R2O, xh)
    send(theirs, RXO, RX_O, d_x)
    for i in range(4):
        recv(R1B.at[0], R2_B + i)
    go_ref[LOW:] = XB[y].astype(F32) + R2B[0].astype(F32) + R2B[1].astype(F32)
    phase("rs_x_wait")
    recv(RXQ, RX_Q)
    gq_ref[...] += RXQ[...].astype(F32)
    recv(RXO, RX_O)
    go_ref[:LOW] += RXO[...].astype(F32)
    phase("perm_wait")
    for k, (b, nb) in enumerate(((5, 1), (4, 1), (2, 2), (0, 2))):
        recv(prev_ref.at[pl.ds(64 * b, 64 * nb)], PERM + k)
    phase("send_wait")
    for cp in started:
        cp.wait_send()
    phase(None)


def local(x, g, a, p, wq, wo, gain, b, w):
    cos, sin = rope_tables()
    any_ = pl.BlockSpec(memory_space=pl.ANY)
    vm = pl.BlockSpec(memory_space=pltpu.VMEM)
    hbm = pl.BlockSpec(memory_space=pltpu.HBM)
    V = pltpu.VMEM
    prev, gq, go = pl.pallas_call(
        kernel,
        name="step",
        out_shape=(
            pltpu.VMEM((SEQ, D), BF),
            pltpu.VMEM((128, QKVW), F32),
            pltpu.VMEM((64, D), F32),
        ),
        in_specs=[any_] * 7 + [hbm] * 2 + [any_] * 2,
        out_specs=(vm, vm, vm),
        scratch_shapes=[
            V((2, SEQ, D), BF), V((2, SEQ, D), BF), V((2, SEQ, QW), BF), V((2, SEQ, QKVW), BF),
            V((CHIPS, 256, QKVW), BF), V((CHIPS, 128, D), BF),
            V((CHIPS, 256, QKVW), BF), V((CHIPS, 128, D), BF),
            V((CHIPS, 128, QKVW), BF), V((CHIPS, 64, D), BF),
            V((2, 128, QKVW), BF), V((2, LOW, D), BF),
            V((2, 2, 128, QKVW), BF), V((2, 2, LOW, D), BF),
            V((128, QKVW), BF), V((LOW, D), BF),
            V((4, XROWS, D), BF), V((2, XROWS, D // 2), BF), V((2, XROWS, D), BF),
            V((SEQ, D), BF), V((SEQ, 128), F32), V((SEQ, QKVW), F32),
            V((KV_HEADS, 6, 256, 128), BF), V((KV_HEADS, 6, 256, 128), BF),
            V((KV_HEADS, SEQ, 128), BF), V((KV_HEADS, SEQ, 128), BF),
            V((128, QKVW), BF), V((KV_HEADS, SEQ, 128), F32), V((KV_HEADS, SEQ, 128), F32),
            V((128, D), F32), V((128, 128), F32), V((SEQ, D), BF),
            V((1, D), F32), V((SEQ, 128), F32), V((SEQ, 128), F32),
            pltpu.SMEM((1,), jnp.int32), pltpu.SMEM((1,), jnp.int32),
            pltpu.SemaphoreType.DMA((11,)),
            pltpu.SemaphoreType.DMA((N_SEM,)),
            pltpu.SemaphoreType.DMA((N_SEM,)),
            pltpu.SemaphoreType.REGULAR,
        ],
        compiler_params=pltpu.CompilerParams(
            collective_id=0, has_side_effects=True, vmem_limit_bytes=59 * 1024 * 1024
        ),
    )(
        x[0], g[0], a[0], p[0], wq[0], wo[0], gain, b, w, jnp.asarray(cos), jnp.asarray(sin)
    )
    return prev[None], gq[None], go[None]


def solution(mesh):
    row = P("section", None, "fsdp", None)
    out = P("section", "fsdp", None)
    return jax.shard_map(
        local,
        mesh=mesh,
        in_specs=(row, row, row, row, out, out, P("section", None), P("section"), P("section")),
        out_specs=(out, out, out),
        check_vma=False,
    )
```

```python
import functools

import jax
import jax.numpy as jnp
import numpy as np
from jax import lax
from jax.experimental import pallas as pl
from jax.experimental.pallas import tpu as pltpu
from jax.sharding import PartitionSpec as P

D = 2048
HEAD_DIM = 64
HEADS = 16
KV_HEADS = 4
SEQ = 384
QW = 1024
QKVW = 1536
CHIPS = 8
EPS = 1e-05
SCALE = HEAD_DIM ** (-0.5)
BF = jnp.bfloat16
F32 = jnp.float32
MESH = pl.DeviceIdType.MESH

Q_X, Q_YP, Q_YM, Q_PP, Q_PM, Q_RO, Q_RP = range(7)
O_YP, O_YM, O_X0, O_XP, O_XM, O_X2, O_RA, O_RB = range(7, 15)
SIB_Q = 15
SIB_O = 23
RS_SIB_Q, RS_SIB_O = 31, 32
R1_Q, R1_O = 33, 35
R2_Q, R2_O = 37, 41
RX_Q, RX_O = 45, 46
PERM = 61
Q_PP2, Q_PM2, Q_RP2 = 51, 52, 53
XB_S = 54
R1_B = 55
R2_B = 57
Q_RO2, SIB_Q6B, SIB_Q7B = 66, 67, 68
N_SEM = 69
XROWS = 16
LOW = 64 - XROWS


def rope_tables():
    half = HEAD_DIM // 2
    freq = 500000.0 ** (-2.0 * np.arange(half) / HEAD_DIM)
    ang = np.arange(SEQ)[:, None] * freq[None, :]
    cos = np.tile(np.cos(ang), (1, 4)).astype(np.float32)
    sin = np.tile(np.sin(ang), (1, 4)).astype(np.float32)
    sign = np.where(np.arange(128) % 64 < 32, -1.0, 1.0).astype(np.float32)
    return cos, sin * sign[None, :]


def dot(a, b, ca, cb):
    return lax.dot_general(a, b, (((ca,), (cb,)), ((), ())), preferred_element_type=F32)


def kernel(
    x_hbm, g_hbm, a_hbm, p_hbm, wq_hbm, wo_hbm, gain_hbm, sched_ref, cos_hbm, sin_hbm,
    prev_ref, gq_ref, go_ref,
    X, G, A, PG, WQ, WO, DQ, DO, SQ, SO, R1Q, R1O, R2Q, R2O, RXQ, RXO, XB, R1B, R2B, WT,
    N, INV, QKV, QS, GS, KD, VD, GP, DK, DV, U, DOT, OUT,
    gain_ref, cos_ref, sin_ref,
    lsem, ssem, rsem, ready,
):
    s = lax.axis_index("section")
    f = lax.axis_index("fsdp")
    xh, y, c = f // 8, (f // 2) % 4, f % 2
    up, down, far = (y + 1) % 4, (y + 3) % 4, (y + 2) % 4
    oc, ox = 1 - c, 1 - xh
    n_sec = lax.axis_size("section")

    def dev(xx, yy, cc):
        return (s, xx * 8 + yy * 2 + cc)

    d_up, d_down, d_x, d_sib = dev(xh, up, c), dev(xh, down, c), dev(ox, y, c), dev(xh, y, oc)
    d_prev, d_next = (lax.rem(s + n_sec - 1, n_sec), f), (lax.rem(s + 1, n_sec), f)

    def qs(ref, xx, yy, cc, lo=0, n=128):
        return ref.at[xx * 4 + yy, pl.ds(pl.multiple_of(cc * 128 + lo, 64), n), :]

    def os(ref, xx, yy, cc, lo=0, n=64):
        return ref.at[xx * 4 + yy, pl.ds(pl.multiple_of(cc * 64 + lo, 16), n), :]

    started = []
    scope = []

    def phase(name):
        if scope:
            scope.pop().__exit__(None, None, None)
        if name:
            scope.append(jax.named_scope(name))
            scope[-1].__enter__()

    def rcopy(src, dst, slot, device):
        return pltpu.make_async_remote_copy(
            src_ref=src, dst_ref=dst, send_sem=ssem.at[slot], recv_sem=rsem.at[slot],
            device_id=device, device_id_type=MESH,
        )

    def send(src, dst, slot, device):
        cp = rcopy(src, dst, slot, device)
        cp.start()
        started.append(cp)

    def recv(dst, slot):
        rcopy(dst, dst, slot, d_sib).wait_recv()

    def gather(ref, shard, slot, device):
        send(shard, shard, slot, device)

    phase("entry")
    barrier = pltpu.get_barrier_semaphore()
    for d in (d_up, d_down, d_x, d_sib, d_prev):
        pl.semaphore_signal(barrier, inc=1, device_id=d, device_id_type=MESH)
    loads = [
        pltpu.make_async_copy(g_hbm, G, lsem.at[0]),
        pltpu.make_async_copy(a_hbm, A, lsem.at[1]),
        pltpu.make_async_copy(x_hbm, X, lsem.at[2]),
        pltpu.make_async_copy(p_hbm, PG, lsem.at[3]),
        pltpu.make_async_copy(wq_hbm, qs(WQ, xh, y, c), lsem.at[4]),
        pltpu.make_async_copy(wo_hbm, os(WO, xh, y, c), lsem.at[5]),
        pltpu.make_async_copy(gain_hbm, gain_ref, lsem.at[6]),
        pltpu.make_async_copy(cos_hbm, cos_ref, lsem.at[7]),
        pltpu.make_async_copy(sin_hbm, sin_ref, lsem.at[8]),
    ]
    for i in (4, 5, 0, 1, 6, 2, 3, 7, 8):
        cp = loads[i]
        cp.start()
    pl.semaphore_wait(barrier, 5)
    pl.semaphore_signal(ready, inc=1, device_id=d_next, device_id_type=MESH)

    phase("own_out")
    mine_q, mine_o = qs(WQ, xh, y, c), os(WO, xh, y, c)
    loads[4].wait()
    gather(WQ, mine_q, Q_YP, d_up)
    gather(WQ, mine_q, Q_YM, d_down)
    gather(WQ, mine_q, Q_X, d_x)
    loads[5].wait()
    gather(WO, mine_o, O_YP, d_up)
    gather(WO, mine_o, O_YM, d_down)
    gather(WO, mine_o, O_X0, d_x)
    gather(WQ, mine_q, SIB_Q + 0, d_sib)
    gather(WO, mine_o, SIB_O + 0, d_sib)

    sched = sched_ref[0]
    b_slot, w_slot = sched % 2, sched // 2

    phase("dw_out")
    loads[0].wait()
    loads[1].wait()

    def out_part(j, carry):
        lhs = A[w_slot, :, pl.ds(pl.multiple_of(j * 256, 256), 256)]
        part = dot(lhs, G[w_slot], 0, 0).astype(BF)
        DO[pl.ds(2 * j, 2)] = part.reshape(2, 128, D)
        return carry

    lax.fori_loop(0, 4, out_part, 0)
    send(DO.at[:, pl.ds(pl.multiple_of(oc * 64, 64), 64), :], SO, RS_SIB_O, d_sib)
    phase("norm_w")
    loads[2].wait()
    loads[3].wait()
    loads[6].wait()

    def norm(slot):
        def rows(r, carry):
            sl = pl.ds(pl.multiple_of(r * 16, 16), 16)
            wide = X[slot, sl, :].astype(F32)
            inv = lax.rsqrt(jnp.mean(wide * wide, axis=-1, keepdims=True) + EPS)
            INV[sl, :] = jnp.broadcast_to(inv, (16, 128))
            N[sl, :] = (wide * inv * gain_ref[...]).astype(BF)
            return carry

        lax.fori_loop(0, SEQ // 16, rows, 0, unroll=4)

    norm(w_slot)

    phase("dw_qkv")

    def qkv_part(j, carry):
        lhs = N[:, pl.ds(pl.multiple_of(j * 256, 256), 256)]
        DQ[j] = dot(lhs, PG[w_slot], 0, 0).astype(BF)
        return carry

    lax.fori_loop(0, CHIPS, qkv_part, 0)
    send(DQ.at[:, pl.ds(pl.multiple_of(oc * 128, 128), 128), :], SQ, RS_SIB_Q, d_sib)
    phase("norm_b")
    norm(b_slot)

    lane = lax.broadcasted_iota(jnp.int32, (128, 128), 1)
    first_half = lane % 64 < 32
    low = lane < 64

    def acc_qkv(xx, yy, first=False):
        j = xx * 4 + yy
        part = dot(N[:, pl.ds(pl.multiple_of(j * 256, 256), 256)], WQ[j], 1, 0)
        QKV[...] = part if first else QKV[...] + part

    def flip(xx, yy, k):
        WT[k] = jnp.transpose(WQ[xx * 4 + yy])

    def stack(ref, b, kv, i, tile):
        zero = jnp.zeros_like(tile)
        ref[kv, b, pl.ds(pl.multiple_of(i * 128, 128), 64)] = jnp.where(low[:64], tile, zero)
        ref[kv, b, pl.ds(pl.multiple_of(i * 128 + 64, 64), 64)] = jnp.where(low[:64], zero, tile)

    def attn_grad(xx, yy):
        j = xx * 4 + yy
        tile = dot(G[b_slot], WO[j], 1, 1).astype(BF)
        for b in range(6):
            stack(GS, b, j // 2, j % 2, tile[b * 64 : (b + 1) * 64])

    def pair_sum_o(j, carry):
        so = pl.ds(pl.multiple_of(c * 64, 64), 64)
        DO[j, so, :] = (DO[j, so, :].astype(F32) + SO[j].astype(F32)).astype(BF)
        return carry

    def pair_sum_q(j, carry):
        sq = pl.ds(pl.multiple_of(c * 128, 128), 128)
        DQ[j, sq, :] = (DQ[j, sq, :].astype(F32) + SQ[j].astype(F32)).astype(BF)
        return carry

    sgn = 1 - 2 * xh
    ya, yb = (y + 4 - sgn) % 4, (y + 4 + sgn) % 4
    phase("fwd_xq")
    part_q = qs(WQ, ox, y, c)
    recv(part_q, Q_X)
    gather(WQ, qs(WQ, ox, y, c, 0, 64), Q_PP, d_up)
    gather(WQ, qs(WQ, ox, y, c, 0, 64), Q_PM, d_down)
    gather(WQ, part_q, SIB_Q + 1, d_sib)
    phase("fwd_yq")
    from_down, from_up = qs(WQ, xh, down, c), qs(WQ, xh, up, c)
    recv(from_down, Q_YP)
    recv(from_up, Q_YM)
    gather(WQ, from_down, SIB_Q + 2, d_sib)
    gather(WQ, from_up, SIB_Q + 3, d_sib)
    phase("sum_o")
    recv(SO, RS_SIB_O)
    lax.fori_loop(0, CHIPS, pair_sum_o, 0)
    phase("qkv_0")
    recv(mine_q, SIB_Q + 0)
    acc_qkv(xh, y, first=True)
    recv(mine_q, SIB_Q + 1)
    acc_qkv(ox, y)
    flip(xh, y, 0)
    flip(ox, y, 1)
    phase("fwd_yo")
    o_down, o_up = os(WO, xh, down, c), os(WO, xh, up, c)
    recv(o_down, O_YP)
    recv(o_up, O_YM)
    gather(WO, os(WO, xh, down, c, 0, 32), O_RA, d_up)
    gather(WO, os(WO, xh, up, c, 32, 32), O_RB, d_down)
    gather(WQ, qs(WQ, ox, y, c, 64, 64), Q_PP2, d_up)
    gather(WQ, qs(WQ, ox, y, c, 64, 64), Q_PM2, d_down)
    gather(WO, o_down, O_XP, d_x)
    gather(WO, o_up, O_XM, d_x)
    gather(WQ, qs(WQ, xh, ya, c, 0, 64), Q_RO, dev(xh, yb, c))
    gather(WQ, qs(WQ, xh, ya, c, 64, 64), Q_RO2, dev(xh, yb, c))
    gather(WO, o_down, SIB_O + 1, d_sib)
    gather(WO, o_up, SIB_O + 2, d_sib)
    o_part = os(WO, ox, y, c)
    recv(o_part, O_X0)
    gather(WO, o_part, SIB_O + 4, d_sib)
    phase("qkv_1")
    recv(mine_q, SIB_Q + 2)
    acc_qkv(xh, down)
    recv(mine_q, SIB_Q + 3)
    acc_qkv(xh, up)
    phase("ag_0")
    recv(mine_o, SIB_O + 0)
    attn_grad(xh, y)
    recv(mine_o, SIB_O + 1)
    attn_grad(xh, down)
    recv(mine_o, SIB_O + 2)
    attn_grad(xh, up)
    recv(mine_o, SIB_O + 4)
    attn_grad(ox, y)
    flip(xh, down, 4)

    phase("fwd_yp1")
    recv(qs(WQ, ox, down, c, 0, 64), Q_PP)
    recv(qs(WQ, ox, up, c, 0, 64), Q_PM)
    gather(WQ, qs(WQ, ox, yb, c, 0, 64), Q_RP, dev(xh, ya, c))
    phase("fwd_ofar")
    o_far = os(WO, xh, far, c)
    recv(os(WO, xh, far, c, 0, 32), O_RA)
    recv(os(WO, xh, far, c, 32, 32), O_RB)
    gather(WO, o_far, O_X2, d_x)
    gather(WO, o_far, SIB_O + 3, d_sib)
    phase("flip_3")
    flip(xh, up, 2)
    phase("fwd_yp")
    part_down, part_up = qs(WQ, ox, down, c), qs(WQ, ox, up, c)
    recv(qs(WQ, ox, down, c, 64, 64), Q_PP2)
    recv(qs(WQ, ox, up, c, 64, 64), Q_PM2)
    gather(WQ, qs(WQ, ox, yb, c, 64, 64), Q_RP2, dev(xh, ya, c))
    gather(WQ, part_down, SIB_Q + 4, d_sib)
    gather(WQ, part_up, SIB_Q + 5, d_sib)

    def pass_o(yy, slot, i):
        piece = os(WO, ox, yy, c)
        recv(piece, slot)
        gather(WO, piece, SIB_O + i, d_sib)

    pass_o(down, O_XP, 5)
    phase("sum_q")
    recv(SQ, RS_SIB_Q)
    lax.fori_loop(0, CHIPS, pair_sum_q, 0)
    send(qs(DQ, 0, far, c), R1Q.at[0], R1_Q + 0, d_up)
    send(qs(DQ, 1, far, c), R1Q.at[1], R1_Q + 1, d_down)
    send(os(DO, 0, far, c, 0, LOW), R1O.at[0], R1_O + 0, d_up)
    send(os(DO, 1, far, c, 0, LOW), R1O.at[1], R1_O + 1, d_down)
    send(qs(DQ, 1, up, c), R2Q.at[0, 1], R2_Q + 1, d_up)
    send(qs(DQ, 0, down, c), R2Q.at[1, 0], R2_Q + 2, d_down)
    phase("ag_1")
    recv(mine_o, SIB_O + 5)
    attn_grad(ox, down)
    phase("qkv_2")
    recv(mine_q, SIB_Q + 4)
    acc_qkv(ox, down)
    recv(mine_q, SIB_Q + 5)
    acc_qkv(ox, up)
    phase("fwd_xo")
    pass_o(up, O_XM, 6)
    send(
        DO.at[pl.ds(ox * 4, 4), pl.ds(pl.multiple_of(c * 64 + LOW, 16), XROWS), :], XB, XB_S, d_x
    )
    phase("ag_2")

    def pass_far(xx, lo, slot, sib):
        piece = qs(WQ, xx, far, c, lo, 64)
        recv(piece, slot)
        gather(WQ, piece, sib, d_sib)

    recv(mine_o, SIB_O + 3)
    attn_grad(xh, far)
    pass_far(xh, 0, Q_RO, SIB_Q + 6)
    pass_far(ox, 0, Q_RP, SIB_Q + 7)
    recv(mine_o, SIB_O + 6)
    attn_grad(ox, up)
    pass_o(far, O_X2, 7)
    phase("flip_45")
    flip(ox, down, 5)
    flip(ox, up, 3)
    phase("fwd_qfar")
    pass_far(xh, 64, Q_RO2, SIB_Q6B)
    pass_far(ox, 64, Q_RP2, SIB_Q7B)
    phase("ag_3")
    recv(mine_o, SIB_O + 7)
    attn_grad(ox, far)
    phase("qkv_3")
    half_q = qs(WQ, xh, y, c, 0, 64)
    recv(half_q, SIB_Q + 6)
    recv(half_q, SIB_Q6B)
    acc_qkv(xh, far)
    recv(half_q, SIB_Q + 7)
    recv(half_q, SIB_Q7B)
    acc_qkv(ox, far)

    phase("rope")
    loads[7].wait()
    loads[8].wait()

    def rot(u):
        mask = first_half[: u.shape[0]]
        return jnp.where(mask, pltpu.roll(u, 96, 1), pltpu.roll(u, 32, 1))

    def rope(u, rows):
        return u * cos_ref[rows, :] + rot(u) * sin_ref[rows, :]

    def unrope(u, rows):
        return u * cos_ref[rows, :] - rot(u) * sin_ref[rows, :]

    def rope_q(b):
        rows = pl.ds(b * 64, 64)
        for t in range(8):
            u = QKV[rows, t * 128 : (t + 1) * 128]
            stack(QS, b, t // 2, t % 2, rope(u, rows).astype(BF))

    for qb in range(3):
        rows = pl.ds(qb * 128, 128)
        for base, dst in ((QW, KD), (QW + 256, VD)):
            for i in range(2):
                u = QKV[rows, base + i * 128 : base + (i + 1) * 128]
                if dst is KD:
                    u = rope(u, rows)
                r = pltpu.roll(u, 64, 1)
                dst[2 * i, rows, :] = jnp.where(low, u, r).astype(BF)
                dst[2 * i + 1, rows, :] = jnp.where(low, r, u).astype(BF)
    rope_q(5)

    exp_scale = SCALE * 1.4426950408889634

    def attend(b0, nb):
        n = nb * 64
        keys = b0 * 64 + n
        rows = pl.ds(b0 * 64, n)
        col = lax.broadcasted_iota(jnp.int32, (n, 4 * n), 1)
        diag = lax.broadcasted_iota(jnp.int32, (n, 4 * n), 0) <= (col // 256) * 64 + col % 64
        low_n = low[:n]

        def one_kv(kv, carry):
            kd, vd = KD[kv, :keys], VD[kv, :keys]
            q4 = QS[kv, b0 : b0 + nb].reshape(4 * n, 128)
            g4 = GS[kv, b0 : b0 + nb].reshape(4 * n, 128)
            e = jnp.exp2(dot(kd, q4, 1, 1) * exp_scale)
            last = jnp.where(diag, e[keys - n :], 0.0)
            e = last if b0 == 0 else jnp.concatenate([e[: keys - n], last], axis=0)
            probs = e * (1.0 / jnp.sum(e, axis=0, keepdims=True))
            dv = dot(probs.astype(BF), g4, 1, 0)
            dp = dot(vd, g4, 1, 1)
            delta = jnp.sum(probs * dp, axis=0, keepdims=True)
            ds = (probs * (dp - delta)).astype(BF)
            dk = dot(ds, q4, 1, 0) * SCALE
            dq = jnp.transpose(dot(kd, ds, 0, 0)) * SCALE
            if keys == SEQ:
                DK[kv], DV[kv] = dk, dv
            else:
                DK[kv, :keys] += dk
                DV[kv, :keys] += dv
            for i in range(2):
                head = [
                    jnp.concatenate(
                        [dq[256 * k + 64 * h : 256 * k + 64 * h + 64] for k in range(nb)], axis=0
                    )
                    for h in (2 * i, 2 * i + 1)
                ]
                sl = pl.ds(pl.multiple_of((2 * kv + i) * 128, 128), 128)
                GP[:n, sl] = unrope(jnp.where(low_n, head[0], head[1]), rows).astype(BF)
            return carry

        lax.fori_loop(0, KV_HEADS, one_kv, 0, unroll=4)
        for i in range(2):
            for base, ref in ((QW, DK), (QW + 256, DV)):
                halves = []
                for kv in (2 * i, 2 * i + 1):
                    t = ref[kv, rows]
                    halves.append(t + pltpu.roll(t, 64, 1))
                tile = jnp.where(low_n, halves[0], halves[1])
                if ref is DK:
                    tile = unrope(tile, rows)
                GP[:n, base + i * 128 : base + (i + 1) * 128] = tile.astype(BF)

    def input_grad(b0, nb, slot):
        n = nb * 64
        rows = pl.ds(b0 * 64, n)
        DOT[...] = jnp.zeros_like(DOT)

        def use(j, u):
            sl = pl.ds(pl.multiple_of(j * 256, 256), 256)
            u = u * gain_ref[:, sl]
            U[:n, sl] = u
            ux = u * X[b_slot, rows, sl].astype(F32)
            DOT[:n] += ux[:, :128] + ux[:, 128:]

        def normed_cols(k, carry):
            t = k // 2
            use((xh + k) % 2 * 4 + (y + t + t // 2) % 4, dot(GP[:n], WT[k], 1, 0))
            return carry

        def far_cols(xx, carry):
            use(xx * 4 + far, dot(GP[:n], WQ[xx * 4 + far], 1, 1))
            return carry

        lax.fori_loop(0, 6, normed_cols, 0, unroll=2)
        lax.fori_loop(0, 2, far_cols, 0, unroll=2)
        phase(f"fin_{b0}")
        inv = INV[rows, :]
        mean = jnp.sum(DOT[:n], axis=-1, keepdims=True) * (1.0 / D)
        DOT[:n] = inv * inv * inv * mean

        def finish(j, carry):
            sl = pl.ds(pl.multiple_of(j * 128, 128), 128)
            for r in range(n // 32):
                part = pl.ds(32 * r, 32)
                here = pl.ds(b0 * 64 + 32 * r, 32)
                res = (
                    G[b_slot, here, sl].astype(F32)
                    + INV[here, :] * U[part, sl]
                    - X[b_slot, here, sl].astype(F32) * DOT[part, :]
                )
                OUT[here, sl] = res.astype(BF)
            return carry

        lax.fori_loop(0, 16, finish, 0, unroll=4)
        if slot == 0:
            pl.semaphore_wait(ready, 1)
        send(OUT.at[rows], prev_ref.at[rows], PERM + slot, d_prev)

    def add_into(dst, other):
        dst[...] = (dst[...].astype(F32) + other.astype(F32)).astype(BF)

    phase("attn_5")
    attend(5, 1)
    phase("ig_5")
    input_grad(5, 1, 0)
    phase("attn_4")
    rope_q(4)
    attend(4, 1)
    phase("ig_4")
    input_grad(4, 1, 1)

    phase("rs_relay_q")
    recv(R1Q.at[0], R1_Q + 0)
    add_into(qs(DQ, 0, up, c), R1Q[0])
    recv(R1Q.at[1], R1_Q + 1)
    add_into(qs(DQ, 1, down, c), R1Q[1])
    send(qs(DQ, 0, up, c), R2Q.at[0, 0], R2_Q + 0, d_up)
    send(qs(DQ, 1, down, c), R2Q.at[1, 1], R2_Q + 3, d_down)
    send(os(DO, 1, up, c, 0, LOW), R2O.at[0, 1], R2_O + 1, d_up)
    send(os(DO, 0, down, c, 0, LOW), R2O.at[1, 0], R2_O + 2, d_down)
    recv(XB, XB_S)
    for i in range(4):
        XB[i] = (XB[i].astype(F32) + os(DO, xh, i, c, LOW, XROWS)[...].astype(F32)).astype(BF)
    c0, c1 = pl.ds(0, D // 2), pl.ds(D // 2, D // 2)
    send(XB.at[far, :, c0], R1B.at[0], R1_B + 0, d_up)
    send(XB.at[far, :, c1], R1B.at[1], R1_B + 1, d_down)
    send(XB.at[up, :, c1], R2B.at[0, :, c1], R2_B + 1, d_up)
    send(XB.at[down, :, c0], R2B.at[1, :, c0], R2_B + 2, d_down)
    phase("attn_3")
    for b in range(4):
        rope_q(b)
    attend(3, 1)
    phase("ig_3")
    input_grad(3, 1, 2)
    phase("attn_2")
    attend(2, 1)
    phase("ig_2")
    input_grad(2, 1, 3)
    phase("rs_relay_o")
    recv(R1O.at[0], R1_O + 0)
    add_into(os(DO, 0, up, c, 0, LOW), R1O[0])
    recv(R1O.at[1], R1_O + 1)
    add_into(os(DO, 1, down, c, 0, LOW), R1O[1])
    send(os(DO, 0, up, c, 0, LOW), R2O.at[0, 0], R2_O + 0, d_up)
    send(os(DO, 1, down, c, 0, LOW), R2O.at[1, 1], R2_O + 3, d_down)
    phase("attn_0")
    attend(0, 2)
    phase("ig_0")
    input_grad(0, 2, 4)

    phase("rs_wait_q")
    for i in range(4):
        recv(R2Q.at[i // 2, i % 2], R2_Q + i)
    phase("rs_tot_q")

    def total(mine, R2, xx):
        return mine[...].astype(F32) + R2[0, xx].astype(F32) + R2[1, xx].astype(F32)

    theirs = qs(DQ, ox, y, c)
    theirs[...] = total(theirs, R2Q, ox).astype(BF)
    gq_ref[...] = total(qs(DQ, xh, y, c), R2Q, xh)
    send(theirs, RXQ, RX_Q, d_x)
    phase("rs_relay_b")
    recv(R1B.at[0], R1_B + 0)
    add_into(XB.at[up, :, c0], R1B[0])
    recv(R1B.at[1], R1_B + 1)
    add_into(XB.at[down, :, c1], R1B[1])
    send(XB.at[up, :, c0], R2B.at[0, :, c0], R2_B + 0, d_up)
    send(XB.at[down, :, c1], R2B.at[1, :, c1], R2_B + 3, d_down)
    phase("rs_wait_o")
    for i in range(4):
        recv(R2O.at[i // 2, i % 2], R2_O + i)
    theirs = os(DO, ox, y, c, 0, LOW)
    theirs[...] = total(theirs, R2O, ox).astype(BF)
    go_ref[:LOW] = total(os(DO, xh, y, c, 0, LOW), R2O, xh)
    send(theirs, RXO, RX_O, d_x)
    for i in range(4):
        recv(R1B.at[0], R2_B + i)
    go_ref[LOW:] = XB[y].astype(F32) + R2B[0].astype(F32) + R2B[1].astype(F32)
    phase("rs_x_wait")
    recv(RXQ, RX_Q)
    gq_ref[...] += RXQ[...].astype(F32)
    recv(RXO, RX_O)
    go_ref[:LOW] += RXO[...].astype(F32)
    phase("perm_wait")
    for k, (b, nb) in enumerate(((5, 1), (4, 1), (3, 1), (2, 1), (0, 2))):
        recv(prev_ref.at[pl.ds(64 * b, 64 * nb)], PERM + k)
    phase("send_wait")
    for cp in started:
        cp.wait_send()
    phase(None)


def local(x, g, a, p, wq, wo, gain, b, w):
    cos, sin = rope_tables()
    any_ = pl.BlockSpec(memory_space=pl.ANY)
    vm = pl.BlockSpec(memory_space=pltpu.VMEM)
    V = pltpu.VMEM
    prev, gq, go = pl.pallas_call(
        kernel,
        name="step",
        out_shape=(
            pltpu.VMEM((SEQ, D), BF),
            pltpu.VMEM((128, QKVW), F32),
            pltpu.VMEM((64, D), F32),
        ),
        in_specs=[any_] * 7 + [pl.BlockSpec(memory_space=pltpu.SMEM)] + [any_] * 2,
        out_specs=(vm, vm, vm),
        scratch_shapes=[
            V((2, SEQ, D), BF), V((2, SEQ, D), BF), V((2, SEQ, QW), BF), V((2, SEQ, QKVW), BF),
            V((CHIPS, 256, QKVW), BF), V((CHIPS, 128, D), BF),
            V((CHIPS, 256, QKVW), BF), V((CHIPS, 128, D), BF),
            V((CHIPS, 128, QKVW), BF), V((CHIPS, 64, D), BF),
            V((2, 128, QKVW), BF), V((2, LOW, D), BF),
            V((2, 2, 128, QKVW), BF), V((2, 2, LOW, D), BF),
            V((128, QKVW), BF), V((LOW, D), BF),
            V((4, XROWS, D), BF), V((2, XROWS, D // 2), BF), V((2, XROWS, D), BF), V((6, QKVW, 256), BF),
            V((SEQ, D), BF), V((SEQ, 128), F32), V((SEQ, QKVW), F32),
            V((KV_HEADS, 6, 256, 128), BF), V((KV_HEADS, 6, 256, 128), BF),
            V((KV_HEADS, SEQ, 128), BF), V((KV_HEADS, SEQ, 128), BF),
            V((128, QKVW), BF), V((KV_HEADS, SEQ, 128), F32), V((KV_HEADS, SEQ, 128), F32),
            V((128, D), F32), V((128, 128), F32), V((SEQ, D), BF),
            V((1, D), F32), V((SEQ, 128), F32), V((SEQ, 128), F32),
            pltpu.SemaphoreType.DMA((9,)),
            pltpu.SemaphoreType.DMA((N_SEM,)),
            pltpu.SemaphoreType.DMA((N_SEM,)),
            pltpu.SemaphoreType.REGULAR,
        ],
        compiler_params=pltpu.CompilerParams(
            collective_id=0, has_side_effects=True, vmem_limit_bytes=59 * 1024 * 1024
        ),
    )(
        x[0], g[0], a[0], p[0], wq[0], wo[0], gain, b + 2 * w,
        jnp.asarray(cos), jnp.asarray(sin),
    )
    return prev[None], gq[None], go[None]


def solution(mesh):
    row = P("section", None, "fsdp", None)
    out = P("section", "fsdp", None)
    return jax.shard_map(
        local,
        mesh=mesh,
        in_specs=(row, row, row, row, out, out, P("section", None), P("section"), P("section")),
        out_specs=(out, out, out),
        check_vma=False,
    )
```

```python
import functools

import jax
import jax.numpy as jnp
import numpy as np
from jax import lax
from jax.experimental import pallas as pl
from jax.experimental.pallas import tpu as pltpu
from jax.sharding import PartitionSpec as P

D = 2048
HEAD_DIM = 64
HEADS = 16
KV_HEADS = 4
SEQ = 384
QW = 1024
QKVW = 1536
CHIPS = 8
EPS = 1e-05
SCALE = HEAD_DIM ** (-0.5)
BF = jnp.bfloat16
F32 = jnp.float32
MESH = pl.DeviceIdType.MESH

Q_X, Q_YP, Q_YM, Q_PP, Q_PM, Q_RO, Q_RP = range(7)
O_YP, O_YM, O_X0, O_XP, O_XM, O_X2, O_RA, O_RB = range(7, 15)
SIB_Q = 15
SIB_O = 23
RS_SIB_Q, RS_SIB_O = 31, 32
R1_Q, R1_O = 33, 35
R2_Q, R2_O = 37, 41
RX_Q, RX_O = 45, 46
PERM = 61
Q_PP2, Q_PM2, Q_RP2 = 51, 52, 53
XB_S = 54
R1_B = 55
R2_B = 57
Q_RO2, SIB_Q6B, SIB_Q7B = 66, 67, 68
N_SEM = 69
XROWS = 16
LOW = 64 - XROWS


def rope_tables():
    half = HEAD_DIM // 2
    freq = 500000.0 ** (-2.0 * np.arange(half) / HEAD_DIM)
    ang = np.arange(SEQ)[:, None] * freq[None, :]
    cos = np.tile(np.cos(ang), (1, 4)).astype(np.float32)
    sin = np.tile(np.sin(ang), (1, 4)).astype(np.float32)
    sign = np.where(np.arange(128) % 64 < 32, -1.0, 1.0).astype(np.float32)
    return cos, sin * sign[None, :]


def dot(a, b, ca, cb):
    return lax.dot_general(a, b, (((ca,), (cb,)), ((), ())), preferred_element_type=F32)


def kernel(
    x_hbm, g_hbm, a_hbm, p_hbm, wq_hbm, wo_hbm, gain_hbm, sched_ref, cos_hbm, sin_hbm,
    prev_ref, gq_ref, go_ref,
    X, G, A, PG, WQ, WO, DQ, DO, SQ, SO, R1Q, R1O, R2Q, R2O, RXQ, RXO, XB, R1B, R2B, WT,
    N, INV, QKV, QS, GS, KD, VD, GP, DK, DV, U, DOT, OUT,
    gain_ref, cos_ref, sin_ref,
    lsem, ssem, rsem, ready,
):
    s = lax.axis_index("section")
    f = lax.axis_index("fsdp")
    xh, y, c = f // 8, (f // 2) % 4, f % 2
    up, down, far = (y + 1) % 4, (y + 3) % 4, (y + 2) % 4
    oc, ox = 1 - c, 1 - xh
    n_sec = lax.axis_size("section")

    def dev(xx, yy, cc):
        return (s, xx * 8 + yy * 2 + cc)

    d_up, d_down, d_x, d_sib = dev(xh, up, c), dev(xh, down, c), dev(ox, y, c), dev(xh, y, oc)
    d_prev, d_next = (lax.rem(s + n_sec - 1, n_sec), f), (lax.rem(s + 1, n_sec), f)

    def qs(ref, xx, yy, cc, lo=0, n=128):
        return ref.at[xx * 4 + yy, pl.ds(pl.multiple_of(cc * 128 + lo, 64), n), :]

    def os(ref, xx, yy, cc, lo=0, n=64):
        return ref.at[xx * 4 + yy, pl.ds(pl.multiple_of(cc * 64 + lo, 16), n), :]

    started = []
    scope = []

    def phase(name):
        if scope:
            scope.pop().__exit__(None, None, None)
        if name:
            scope.append(jax.named_scope(name))
            scope[-1].__enter__()

    def rcopy(src, dst, slot, device):
        return pltpu.make_async_remote_copy(
            src_ref=src, dst_ref=dst, send_sem=ssem.at[slot], recv_sem=rsem.at[slot],
            device_id=device, device_id_type=MESH,
        )

    def send(src, dst, slot, device):
        cp = rcopy(src, dst, slot, device)
        cp.start()
        started.append(cp)

    def recv(dst, slot):
        rcopy(dst, dst, slot, d_sib).wait_recv()

    def gather(ref, shard, slot, device):
        send(shard, shard, slot, device)

    phase("entry")
    barrier = pltpu.get_barrier_semaphore()
    for d in (d_up, d_down, d_x, d_sib, d_prev):
        pl.semaphore_signal(barrier, inc=1, device_id=d, device_id_type=MESH)
    loads = [
        pltpu.make_async_copy(g_hbm, G, lsem.at[0]),
        pltpu.make_async_copy(a_hbm, A, lsem.at[1]),
        pltpu.make_async_copy(x_hbm, X, lsem.at[2]),
        pltpu.make_async_copy(p_hbm, PG, lsem.at[3]),
        pltpu.make_async_copy(wq_hbm, qs(WQ, xh, y, c), lsem.at[4]),
        pltpu.make_async_copy(wo_hbm, os(WO, xh, y, c), lsem.at[5]),
        pltpu.make_async_copy(gain_hbm, gain_ref, lsem.at[6]),
        pltpu.make_async_copy(cos_hbm, cos_ref, lsem.at[7]),
        pltpu.make_async_copy(sin_hbm, sin_ref, lsem.at[8]),
    ]
    for i in (4, 5, 0, 1, 6, 2, 3, 7, 8):
        cp = loads[i]
        cp.start()
    pl.semaphore_wait(barrier, 5)
    pl.semaphore_signal(ready, inc=1, device_id=d_next, device_id_type=MESH)

    phase("own_out")
    mine_q, mine_o = qs(WQ, xh, y, c), os(WO, xh, y, c)
    loads[4].wait()
    gather(WQ, mine_q, Q_YP, d_up)
    gather(WQ, mine_q, Q_YM, d_down)
    gather(WQ, mine_q, Q_X, d_x)
    loads[5].wait()
    gather(WO, mine_o, O_YP, d_up)
    gather(WO, mine_o, O_YM, d_down)
    gather(WO, mine_o, O_X0, d_x)
    gather(WQ, mine_q, SIB_Q + 0, d_sib)
    gather(WO, mine_o, SIB_O + 0, d_sib)

    sched = sched_ref[0]
    b_slot, w_slot = sched % 2, sched // 2

    phase("dw_out")
    loads[0].wait()
    loads[1].wait()

    def out_part(j, carry):
        lhs = A[w_slot, :, pl.ds(pl.multiple_of(j * 256, 256), 256)]
        part = dot(lhs, G[w_slot], 0, 0).astype(BF)
        DO[pl.ds(2 * j, 2)] = part.reshape(2, 128, D)
        return carry

    lax.fori_loop(0, 4, out_part, 0)
    send(DO.at[:, pl.ds(pl.multiple_of(oc * 64, 64), 64), :], SO, RS_SIB_O, d_sib)
    phase("norm_w")
    loads[2].wait()
    loads[3].wait()
    loads[6].wait()

    def norm(slot):
        def rows(r, carry):
            sl = pl.ds(pl.multiple_of(r * 16, 16), 16)
            wide = X[slot, sl, :].astype(F32)
            inv = lax.rsqrt(jnp.mean(wide * wide, axis=-1, keepdims=True) + EPS)
            INV[sl, :] = jnp.broadcast_to(inv, (16, 128))
            N[sl, :] = (wide * inv * gain_ref[...]).astype(BF)
            return carry

        lax.fori_loop(0, SEQ // 16, rows, 0, unroll=4)

    norm(w_slot)

    phase("dw_qkv")

    def qkv_part(j, carry):
        lhs = N[:, pl.ds(pl.multiple_of(j * 256, 256), 256)]
        DQ[j] = dot(lhs, PG[w_slot], 0, 0).astype(BF)
        return carry

    lax.fori_loop(0, CHIPS, qkv_part, 0)
    send(DQ.at[:, pl.ds(pl.multiple_of(oc * 128, 128), 128), :], SQ, RS_SIB_Q, d_sib)
    phase("norm_b")
    norm(b_slot)

    lane = lax.broadcasted_iota(jnp.int32, (128, 128), 1)
    first_half = lane % 64 < 32
    low = lane < 64

    def acc_qkv(xx, yy, first=False):
        j = xx * 4 + yy
        part = dot(N[:, pl.ds(pl.multiple_of(j * 256, 256), 256)], WQ[j], 1, 0)
        QKV[...] = part if first else QKV[...] + part

    def flip(xx, yy, k):
        WT[k] = jnp.transpose(WQ[xx * 4 + yy])

    def stack(ref, b, kv, i, tile):
        zero = jnp.zeros_like(tile)
        ref[kv, b, pl.ds(pl.multiple_of(i * 128, 128), 64)] = jnp.where(low[:64], tile, zero)
        ref[kv, b, pl.ds(pl.multiple_of(i * 128 + 64, 64), 64)] = jnp.where(low[:64], zero, tile)

    def attn_grad(xx, yy):
        j = xx * 4 + yy
        tile = dot(G[b_slot], WO[j], 1, 1).astype(BF)
        for b in range(6):
            stack(GS, b, j // 2, j % 2, tile[b * 64 : (b + 1) * 64])

    def pair_sum_o(j, carry):
        so = pl.ds(pl.multiple_of(c * 64, 64), 64)
        DO[j, so, :] = (DO[j, so, :].astype(F32) + SO[j].astype(F32)).astype(BF)
        return carry

    def pair_sum_q(j, carry):
        sq = pl.ds(pl.multiple_of(c * 128, 128), 128)
        DQ[j, sq, :] = (DQ[j, sq, :].astype(F32) + SQ[j].astype(F32)).astype(BF)
        return carry

    sgn = 1 - 2 * xh
    ya, yb = (y + 4 - sgn) % 4, (y + 4 + sgn) % 4
    phase("fwd_xq")
    part_q = qs(WQ, ox, y, c)
    recv(part_q, Q_X)
    gather(WQ, qs(WQ, ox, y, c, 0, 64), Q_PP, d_up)
    gather(WQ, qs(WQ, ox, y, c, 0, 64), Q_PM, d_down)
    gather(WQ, part_q, SIB_Q + 1, d_sib)
    phase("fwd_yq")
    from_down, from_up = qs(WQ, xh, down, c), qs(WQ, xh, up, c)
    recv(from_down, Q_YP)
    recv(from_up, Q_YM)
    gather(WQ, from_down, SIB_Q + 2, d_sib)
    gather(WQ, from_up, SIB_Q + 3, d_sib)
    phase("sum_o")
    recv(SO, RS_SIB_O)
    lax.fori_loop(0, CHIPS, pair_sum_o, 0)
    phase("qkv_0")
    recv(mine_q, SIB_Q + 0)
    acc_qkv(xh, y, first=True)
    recv(mine_q, SIB_Q + 1)
    acc_qkv(ox, y)
    flip(xh, y, 0)
    flip(ox, y, 1)
    phase("fwd_yo")
    o_down, o_up = os(WO, xh, down, c), os(WO, xh, up, c)
    recv(o_down, O_YP)
    recv(o_up, O_YM)
    gather(WO, os(WO, xh, down, c, 0, 32), O_RA, d_up)
    gather(WO, os(WO, xh, up, c, 32, 32), O_RB, d_down)
    gather(WQ, qs(WQ, ox, y, c, 64, 64), Q_PP2, d_up)
    gather(WQ, qs(WQ, ox, y, c, 64, 64), Q_PM2, d_down)
    gather(WO, o_down, O_XP, d_x)
    gather(WO, o_up, O_XM, d_x)
    gather(WQ, qs(WQ, xh, ya, c, 0, 64), Q_RO, dev(xh, yb, c))
    gather(WQ, qs(WQ, xh, ya, c, 64, 64), Q_RO2, dev(xh, yb, c))
    gather(WO, o_down, SIB_O + 1, d_sib)
    gather(WO, o_up, SIB_O + 2, d_sib)
    o_part = os(WO, ox, y, c)
    recv(o_part, O_X0)
    gather(WO, o_part, SIB_O + 4, d_sib)
    phase("qkv_1")
    recv(mine_q, SIB_Q + 2)
    acc_qkv(xh, down)
    recv(mine_q, SIB_Q + 3)
    acc_qkv(xh, up)
    phase("ag_0")
    recv(mine_o, SIB_O + 0)
    attn_grad(xh, y)
    recv(mine_o, SIB_O + 1)
    attn_grad(xh, down)
    recv(mine_o, SIB_O + 2)
    attn_grad(xh, up)
    recv(mine_o, SIB_O + 4)
    attn_grad(ox, y)
    flip(xh, down, 4)

    phase("fwd_yp1")
    recv(qs(WQ, ox, down, c, 0, 64), Q_PP)
    recv(qs(WQ, ox, up, c, 0, 64), Q_PM)
    gather(WQ, qs(WQ, ox, yb, c, 0, 64), Q_RP, dev(xh, ya, c))
    phase("fwd_ofar")
    o_far = os(WO, xh, far, c)
    recv(os(WO, xh, far, c, 0, 32), O_RA)
    recv(os(WO, xh, far, c, 32, 32), O_RB)
    gather(WO, o_far, O_X2, d_x)
    gather(WO, o_far, SIB_O + 3, d_sib)
    phase("flip_3")
    flip(xh, up, 2)
    phase("fwd_yp")
    part_down, part_up = qs(WQ, ox, down, c), qs(WQ, ox, up, c)
    recv(qs(WQ, ox, down, c, 64, 64), Q_PP2)
    recv(qs(WQ, ox, up, c, 64, 64), Q_PM2)
    gather(WQ, qs(WQ, ox, yb, c, 64, 64), Q_RP2, dev(xh, ya, c))
    gather(WQ, part_down, SIB_Q + 4, d_sib)
    gather(WQ, part_up, SIB_Q + 5, d_sib)

    def pass_o(yy, slot, i):
        piece = os(WO, ox, yy, c)
        recv(piece, slot)
        gather(WO, piece, SIB_O + i, d_sib)

    pass_o(down, O_XP, 5)
    phase("sum_q")
    recv(SQ, RS_SIB_Q)
    lax.fori_loop(0, CHIPS, pair_sum_q, 0)
    send(qs(DQ, 0, far, c), R1Q.at[0], R1_Q + 0, d_up)
    send(qs(DQ, 1, far, c), R1Q.at[1], R1_Q + 1, d_down)
    send(os(DO, 0, far, c, 0, LOW), R1O.at[0], R1_O + 0, d_up)
    send(os(DO, 1, far, c, 0, LOW), R1O.at[1], R1_O + 1, d_down)
    send(qs(DQ, 1, up, c), R2Q.at[0, 1], R2_Q + 1, d_up)
    send(qs(DQ, 0, down, c), R2Q.at[1, 0], R2_Q + 2, d_down)
    phase("ag_1")
    recv(mine_o, SIB_O + 5)
    attn_grad(ox, down)
    phase("qkv_2")
    recv(mine_q, SIB_Q + 4)
    acc_qkv(ox, down)
    recv(mine_q, SIB_Q + 5)
    acc_qkv(ox, up)
    phase("fwd_xo")
    pass_o(up, O_XM, 6)
    send(
        DO.at[pl.ds(ox * 4, 4), pl.ds(pl.multiple_of(c * 64 + LOW, 16), XROWS), :], XB, XB_S, d_x
    )
    phase("ag_2")

    def pass_far(xx, lo, slot, sib):
        piece = qs(WQ, xx, far, c, lo, 64)
        recv(piece, slot)
        gather(WQ, piece, sib, d_sib)

    recv(mine_o, SIB_O + 3)
    attn_grad(xh, far)
    pass_far(xh, 0, Q_RO, SIB_Q + 6)
    pass_far(ox, 0, Q_RP, SIB_Q + 7)
    recv(mine_o, SIB_O + 6)
    attn_grad(ox, up)
    pass_o(far, O_X2, 7)
    phase("flip_45")
    flip(ox, down, 5)
    flip(ox, up, 3)
    phase("fwd_qfar")
    pass_far(xh, 64, Q_RO2, SIB_Q6B)
    pass_far(ox, 64, Q_RP2, SIB_Q7B)
    phase("ag_3")
    recv(mine_o, SIB_O + 7)
    attn_grad(ox, far)
    phase("qkv_3")
    half_q = qs(WQ, xh, y, c, 0, 64)
    recv(half_q, SIB_Q + 6)
    recv(half_q, SIB_Q6B)
    acc_qkv(xh, far)
    recv(half_q, SIB_Q + 7)
    recv(half_q, SIB_Q7B)
    acc_qkv(ox, far)

    phase("rope")
    loads[7].wait()
    loads[8].wait()

    def rot(u):
        mask = first_half[: u.shape[0]]
        return jnp.where(mask, pltpu.roll(u, 96, 1), pltpu.roll(u, 32, 1))

    def rope(u, rows):
        return u * cos_ref[rows, :] + rot(u) * sin_ref[rows, :]

    def unrope(u, rows):
        return u * cos_ref[rows, :] - rot(u) * sin_ref[rows, :]

    def rope_q(b):
        rows = pl.ds(b * 64, 64)
        for t in range(8):
            u = QKV[rows, t * 128 : (t + 1) * 128]
            stack(QS, b, t // 2, t % 2, rope(u, rows).astype(BF))

    for qb in range(3):
        rows = pl.ds(qb * 128, 128)
        for base, dst in ((QW, KD), (QW + 256, VD)):
            for i in range(2):
                u = QKV[rows, base + i * 128 : base + (i + 1) * 128]
                if dst is KD:
                    u = rope(u, rows)
                r = pltpu.roll(u, 64, 1)
                dst[2 * i, rows, :] = jnp.where(low, u, r).astype(BF)
                dst[2 * i + 1, rows, :] = jnp.where(low, r, u).astype(BF)
    rope_q(5)

    exp_scale = SCALE * 1.4426950408889634

    def attend(b0, nb):
        n = nb * 64
        keys = b0 * 64 + n
        rows = pl.ds(b0 * 64, n)
        col = lax.broadcasted_iota(jnp.int32, (n, 4 * n), 1)
        diag = lax.broadcasted_iota(jnp.int32, (n, 4 * n), 0) <= (col // 256) * 64 + col % 64
        low_n = low[:n]

        def one_kv(kv, carry):
            kd, vd = KD[kv, :keys], VD[kv, :keys]
            q4 = QS[kv, b0 : b0 + nb].reshape(4 * n, 128)
            g4 = GS[kv, b0 : b0 + nb].reshape(4 * n, 128)
            e = jnp.exp2(dot(kd, q4, 1, 1) * exp_scale)
            last = jnp.where(diag, e[keys - n :], 0.0)
            e = last if b0 == 0 else jnp.concatenate([e[: keys - n], last], axis=0)
            probs = e * (1.0 / jnp.sum(e, axis=0, keepdims=True))
            dv = dot(probs.astype(BF), g4, 1, 0)
            dp = dot(vd, g4, 1, 1)
            delta = jnp.sum(probs * dp, axis=0, keepdims=True)
            ds = (probs * (dp - delta)).astype(BF)
            dk = dot(ds, q4, 1, 0) * SCALE
            dq = jnp.transpose(dot(kd, ds, 0, 0)) * SCALE
            if keys == SEQ:
                DK[kv], DV[kv] = dk, dv
            else:
                DK[kv, :keys] += dk
                DV[kv, :keys] += dv
            for i in range(2):
                head = [
                    jnp.concatenate(
                        [dq[256 * k + 64 * h : 256 * k + 64 * h + 64] for k in range(nb)], axis=0
                    )
                    for h in (2 * i, 2 * i + 1)
                ]
                sl = pl.ds(pl.multiple_of((2 * kv + i) * 128, 128), 128)
                GP[:n, sl] = unrope(jnp.where(low_n, head[0], head[1]), rows).astype(BF)
            return carry

        lax.fori_loop(0, KV_HEADS, one_kv, 0, unroll=4)
        for i in range(2):
            for base, ref in ((QW, DK), (QW + 256, DV)):
                halves = []
                for kv in (2 * i, 2 * i + 1):
                    t = ref[kv, rows]
                    halves.append(t + pltpu.roll(t, 64, 1))
                tile = jnp.where(low_n, halves[0], halves[1])
                if ref is DK:
                    tile = unrope(tile, rows)
                GP[:n, base + i * 128 : base + (i + 1) * 128] = tile.astype(BF)

    def input_grad(b0, nb, slot):
        n = nb * 64
        rows = pl.ds(b0 * 64, n)
        DOT[...] = jnp.zeros_like(DOT)

        def use(j, u):
            sl = pl.ds(pl.multiple_of(j * 256, 256), 256)
            u = u * gain_ref[:, sl]
            U[:n, sl] = u
            ux = u * X[b_slot, rows, sl].astype(F32)
            DOT[:n] += ux[:, :128] + ux[:, 128:]

        def normed_cols(k, carry):
            t = k // 2
            use((xh + k) % 2 * 4 + (y + t + t // 2) % 4, dot(GP[:n], WT[k], 1, 0))
            return carry

        def far_cols(xx, carry):
            use(xx * 4 + far, dot(GP[:n], WQ[xx * 4 + far], 1, 1))
            return carry

        lax.fori_loop(0, 6, normed_cols, 0, unroll=3)
        lax.fori_loop(0, 2, far_cols, 0, unroll=2)
        phase(f"fin_{b0}")
        inv = INV[rows, :]
        mean = jnp.sum(DOT[:n], axis=-1, keepdims=True) * (1.0 / D)
        DOT[:n] = inv * inv * inv * mean

        def finish(j, carry):
            sl = pl.ds(pl.multiple_of(j * 128, 128), 128)
            for r in range(n // 32):
                part = pl.ds(32 * r, 32)
                here = pl.ds(b0 * 64 + 32 * r, 32)
                res = (
                    G[b_slot, here, sl].astype(F32)
                    + INV[here, :] * U[part, sl]
                    - X[b_slot, here, sl].astype(F32) * DOT[part, :]
                )
                OUT[here, sl] = res.astype(BF)
            return carry

        lax.fori_loop(0, 16, finish, 0, unroll=4)
        if slot == 0:
            pl.semaphore_wait(ready, 1)
        send(OUT.at[rows], prev_ref.at[rows], PERM + slot, d_prev)

    def add_into(dst, other):
        dst[...] = (dst[...].astype(F32) + other.astype(F32)).astype(BF)

    phase("attn_5")
    attend(5, 1)
    phase("ig_5")
    input_grad(5, 1, 0)
    phase("attn_4")
    rope_q(4)
    attend(4, 1)
    phase("ig_4")
    input_grad(4, 1, 1)

    phase("rs_relay_q")
    recv(R1Q.at[0], R1_Q + 0)
    add_into(qs(DQ, 0, up, c), R1Q[0])
    recv(R1Q.at[1], R1_Q + 1)
    add_into(qs(DQ, 1, down, c), R1Q[1])
    send(qs(DQ, 0, up, c), R2Q.at[0, 0], R2_Q + 0, d_up)
    send(qs(DQ, 1, down, c), R2Q.at[1, 1], R2_Q + 3, d_down)
    send(os(DO, 1, up, c, 0, LOW), R2O.at[0, 1], R2_O + 1, d_up)
    send(os(DO, 0, down, c, 0, LOW), R2O.at[1, 0], R2_O + 2, d_down)
    recv(XB, XB_S)
    for i in range(4):
        XB[i] = (XB[i].astype(F32) + os(DO, xh, i, c, LOW, XROWS)[...].astype(F32)).astype(BF)
    c0, c1 = pl.ds(0, D // 2), pl.ds(D // 2, D // 2)
    send(XB.at[far, :, c0], R1B.at[0], R1_B + 0, d_up)
    send(XB.at[far, :, c1], R1B.at[1], R1_B + 1, d_down)
    send(XB.at[up, :, c1], R2B.at[0, :, c1], R2_B + 1, d_up)
    send(XB.at[down, :, c0], R2B.at[1, :, c0], R2_B + 2, d_down)
    phase("attn_3")
    for b in range(4):
        rope_q(b)
    attend(3, 1)
    phase("ig_3")
    input_grad(3, 1, 2)
    phase("attn_2")
    attend(2, 1)
    phase("ig_2")
    input_grad(2, 1, 3)
    phase("rs_relay_o")
    recv(R1O.at[0], R1_O + 0)
    add_into(os(DO, 0, up, c, 0, LOW), R1O[0])
    recv(R1O.at[1], R1_O + 1)
    add_into(os(DO, 1, down, c, 0, LOW), R1O[1])
    send(os(DO, 0, up, c, 0, LOW), R2O.at[0, 0], R2_O + 0, d_up)
    send(os(DO, 1, down, c, 0, LOW), R2O.at[1, 1], R2_O + 3, d_down)
    phase("attn_0")
    attend(0, 2)
    phase("ig_0")
    input_grad(0, 2, 4)

    phase("rs_wait_q")
    for i in range(4):
        recv(R2Q.at[i // 2, i % 2], R2_Q + i)
    phase("rs_tot_q")

    def total(mine, R2, xx):
        return mine[...].astype(F32) + R2[0, xx].astype(F32) + R2[1, xx].astype(F32)

    theirs = qs(DQ, ox, y, c)
    theirs[...] = total(theirs, R2Q, ox).astype(BF)
    gq_ref[...] = total(qs(DQ, xh, y, c), R2Q, xh)
    send(theirs, RXQ, RX_Q, d_x)
    phase("rs_relay_b")
    recv(R1B.at[0], R1_B + 0)
    add_into(XB.at[up, :, c0], R1B[0])
    recv(R1B.at[1], R1_B + 1)
    add_into(XB.at[down, :, c1], R1B[1])
    send(XB.at[up, :, c0], R2B.at[0, :, c0], R2_B + 0, d_up)
    send(XB.at[down, :, c1], R2B.at[1, :, c1], R2_B + 3, d_down)
    phase("rs_wait_o")
    for i in range(4):
        recv(R2O.at[i // 2, i % 2], R2_O + i)
    theirs = os(DO, ox, y, c, 0, LOW)
    theirs[...] = total(theirs, R2O, ox).astype(BF)
    go_ref[:LOW] = total(os(DO, xh, y, c, 0, LOW), R2O, xh)
    send(theirs, RXO, RX_O, d_x)
    for i in range(4):
        recv(R1B.at[0], R2_B + i)
    go_ref[LOW:] = XB[y].astype(F32) + R2B[0].astype(F32) + R2B[1].astype(F32)
    phase("rs_x_wait")
    recv(RXQ, RX_Q)
    gq_ref[...] += RXQ[...].astype(F32)
    recv(RXO, RX_O)
    go_ref[:LOW] += RXO[...].astype(F32)
    phase("perm_wait")
    for k, (b, nb) in enumerate(((5, 1), (4, 1), (3, 1), (2, 1), (0, 2))):
        recv(prev_ref.at[pl.ds(64 * b, 64 * nb)], PERM + k)
    phase("send_wait")
    for cp in started:
        cp.wait_send()
    phase(None)


def local(x, g, a, p, wq, wo, gain, b, w):
    cos, sin = rope_tables()
    any_ = pl.BlockSpec(memory_space=pl.ANY)
    vm = pl.BlockSpec(memory_space=pltpu.VMEM)
    V = pltpu.VMEM
    prev, gq, go = pl.pallas_call(
        kernel,
        name="step",
        out_shape=(
            pltpu.VMEM((SEQ, D), BF),
            pltpu.VMEM((128, QKVW), F32),
            pltpu.VMEM((64, D), F32),
        ),
        in_specs=[any_] * 7 + [pl.BlockSpec(memory_space=pltpu.SMEM)] + [any_] * 2,
        out_specs=(vm, vm, vm),
        scratch_shapes=[
            V((2, SEQ, D), BF), V((2, SEQ, D), BF), V((2, SEQ, QW), BF), V((2, SEQ, QKVW), BF),
            V((CHIPS, 256, QKVW), BF), V((CHIPS, 128, D), BF),
            V((CHIPS, 256, QKVW), BF), V((CHIPS, 128, D), BF),
            V((CHIPS, 128, QKVW), BF), V((CHIPS, 64, D), BF),
            V((2, 128, QKVW), BF), V((2, LOW, D), BF),
            V((2, 2, 128, QKVW), BF), V((2, 2, LOW, D), BF),
            V((128, QKVW), BF), V((LOW, D), BF),
            V((4, XROWS, D), BF), V((2, XROWS, D // 2), BF), V((2, XROWS, D), BF), V((6, QKVW, 256), BF),
            V((SEQ, D), BF), V((SEQ, 128), F32), V((SEQ, QKVW), F32),
            V((KV_HEADS, 6, 256, 128), BF), V((KV_HEADS, 6, 256, 128), BF),
            V((KV_HEADS, SEQ, 128), BF), V((KV_HEADS, SEQ, 128), BF),
            V((128, QKVW), BF), V((KV_HEADS, SEQ, 128), F32), V((KV_HEADS, SEQ, 128), F32),
            V((128, D), F32), V((128, 128), F32), V((SEQ, D), BF),
            V((1, D), F32), V((SEQ, 128), F32), V((SEQ, 128), F32),
            pltpu.SemaphoreType.DMA((9,)),
            pltpu.SemaphoreType.DMA((N_SEM,)),
            pltpu.SemaphoreType.DMA((N_SEM,)),
            pltpu.SemaphoreType.REGULAR,
        ],
        compiler_params=pltpu.CompilerParams(
            collective_id=0, has_side_effects=True, vmem_limit_bytes=59 * 1024 * 1024
        ),
    )(
        x[0], g[0], a[0], p[0], wq[0], wo[0], gain, b + 2 * w,
        jnp.asarray(cos), jnp.asarray(sin),
    )
    return prev[None], gq[None], go[None]


def solution(mesh):
    row = P("section", None, "fsdp", None)
    out = P("section", "fsdp", None)
    return jax.shard_map(
        local,
        mesh=mesh,
        in_specs=(row, row, row, row, out, out, P("section", None), P("section"), P("section")),
        out_specs=(out, out, out),
        check_vma=False,
    )
```
